128 devices in a mesh: gx: 32 (over y, z, core), gy: 4 (over x).
Axes of the slice: x: 4, y: 4, z: 4, core: 2. Of those that a mesh axis runs over, the one named last changes fastest.
Arguments:
- velocity: bfloat16 [3, 64, 16, 16, 512], P(None, 'gx', 'gy'), may hold values from -6 to 6
- part_pos: float32 [16384, 3, 128], P(('gx', 'gy')), may hold values from -1 to 1
- part_vel: float32 [16384, 3, 128], P(('gx', 'gy')), may hold values from -6 to 6
- part_coef: float32 [16384, 2, 128], P(('gx', 'gy')), may hold values from 0.3 to 3
- counts: int32 [16384], P(('gx', 'gy')), may hold values from 1 to 128
- dest: int32 [16384], P(('gx', 'gy')), may hold values from 0 to 3, as said below
- elem: int32 [16384], P(('gx', 'gy')), may hold values from 0 to 127, as said below
Outputs:
- drag: float32 [16384, 3, 128], P(('gx', 'gy'))
- source: float32 [3, 64, 16, 16, 512], P(None, 'gx', 'gy')
The draws below stay inside these ranges and needn't reach their ends.
Inputs may be any that keep to these rules, and one draw needn't show every extreme that they name: `dest`: every device sends exactly 32 blocks to each gy index. `elem`: on every owning device, each of its 128 elements receives exactly one block.
All inputs are finite; a program needn't handle non-finite values.
Results may differ from the reference program's by a relative error of at most 0.0003.
Values sent between devices are 32-bit elements; how exact they have to be, the bound alone decides.
A program may use at most 128 MiB of HBM per device.

```python
import math
import jax
import jax.numpy as jnp
from jax import lax

EXD = 2
EYD = 4
EZ = 16
NODES = 512
SLOTS = 128
E_DEV = 128
NEX = 64
NEY = 16
NB = 16384
N_GX = 32
N_GY = 4


def joint_routes(key):
    share_size = E_DEV // N_GY

    def one_row(row_key):
        elem_keys = jax.random.split(jax.random.fold_in(row_key, 1), N_GY)
        mix_keys = jax.random.split(jax.random.fold_in(row_key, 2), N_GY)
        ladder = jnp.arange(E_DEV, dtype=jnp.int32)
        incoming = jax.vmap(lambda k: jax.random.permutation(k, ladder))(elem_keys)
        elements = incoming.reshape(N_GY, N_GY, share_size).transpose(1, 0, 2).reshape(N_GY, E_DEV)
        targets = jnp.broadcast_to(jnp.arange(N_GY, dtype=jnp.int32)[None, :, None], (N_GY, N_GY, share_size)).reshape(N_GY, E_DEV)
        shuffle = jax.vmap(lambda k: jax.random.permutation(k, ladder))(mix_keys)
        return (jnp.take_along_axis(targets, shuffle, axis=1), jnp.take_along_axis(elements, shuffle, axis=1))
    targets, elements = jax.vmap(one_row)(jax.random.split(key, N_GX))
    return (targets.reshape(-1), elements.reshape(-1))


def draw_dest(key, part):
    return joint_routes(jax.random.fold_in(key, 7))[0]


def draw_elem(key, part):
    return joint_routes(jax.random.fold_in(key, 7))[1]


def set_ends(result, stream_key, low, high):
    extent = result.shape
    spot = [jax.random.randint(jax.random.fold_in(stream_key, axis), (), 0, extent[axis]) for axis in range(len(extent))]
    result = result.at[tuple(spot)].set(low)
    longest = extent.index(max(extent))
    spot[longest] = (spot[longest] + 1) % extent[longest]
    return result.at[tuple(spot)].set(high)


def block_scale(stream_key, extent, pieces, smallest, largest):
    def one(dim, parts):
        steps = jax.random.uniform(jax.random.fold_in(jax.random.fold_in(stream_key, 6), dim), (parts,), jnp.float32, smallest / len(pieces), largest / len(pieces))
        return jnp.repeat(jnp.exp(steps), extent[dim] // parts).reshape((-1,) + (1,) * (len(extent) - dim - 1))

    loudness = one(*pieces[0])
    for cut in pieces[1:]:
        loudness = loudness * one(*cut)
    return loudness


def scatter_about(key, shape, scale, most, cuts=(), kind=jnp.bfloat16):
    level = block_scale(key, shape, cuts, -0.22, 0.18) if cuts else 1.0
    drawn = jax.random.normal(key, shape, jnp.float32) * scale * level
    return jnp.minimum(jnp.maximum(drawn, -most), most).astype(kind)


def setup_inputs(seed: int = 0) -> dict:
    splits = jax.random.split(jax.random.key(seed), 8)
    return {
        "velocity": scatter_about(splits[0], (3, NEX, NEY, EZ, NODES), 1.0, 6.0, ((1, 32), (2, 4))),
        "part_pos": jnp.clip(jax.random.uniform(splits[1], (NB, 3, SLOTS), jnp.float32, -1.0, 1.0) * block_scale(splits[1], (NB, 3, SLOTS), ((0, 128),), -0.4, 0.0), -1.0, 1.0),
        "part_vel": scatter_about(splits[2], (NB, 3, SLOTS), 1.0, 6.0, ((0, 128),), jnp.float32),
        "part_coef": jnp.clip(jnp.exp(math.log(3.0) - 2.3025851 * jax.random.uniform(splits[3], (NB, 2, SLOTS), jnp.float32) ** block_scale(splits[3], (NB, 2, SLOTS), ((0, 128),), -0.2, 0.2)), 0.3, 3.0),
        "counts": set_ends(jax.random.randint(splits[4], (NB,), 1, 129), jax.random.fold_in(splits[4], 1), 1, 128).astype(jnp.int32),
        "dest": draw_dest(jax.random.fold_in(splits[7], 71), 0),
        "elem": draw_elem(jax.random.fold_in(splits[7], 71), 0),
    }


GLL = (-1.0, -0.8717401485096066, -0.5917001814331423, -0.2092992179024789, 0.2092992179024789, 0.5917001814331423, 0.8717401485096066, 1.0)
HIGH = lax.Precision.HIGHEST
SHARPNESS = 8.0

def lagrange_rows(coord):
    layers = []
    for i in range(8):
        product = jnp.ones_like(coord)
        for m in range(8):
            if m != i:
                product = product * ((coord - GLL[m]) / (GLL[i] - GLL[m]))
        layers.append(product)
    return jnp.stack(layers, axis=1)

def gauss_rows(coord, offset):
    points = jnp.array(GLL, dtype=jnp.float32)
    spacing = points[None, :, None] - (coord[:, None, :] + offset)
    return jnp.exp(-SHARPNESS * spacing * spacing)

def element_step(field, position, carried, coefs, filled):
    group = field.shape[0]
    width = position.shape[2]
    basis_r = lagrange_rows(position[:, 0])
    basis_s = lagrange_rows(position[:, 1])
    basis_t = lagrange_rows(position[:, 2])
    nodal = field.reshape(group, 3, 8, 64)
    partial_sum = jnp.einsum('gcia,gip->gcap', nodal, basis_r, precision=HIGH)
    planes = (basis_s[:, :, None, :] * basis_t[:, None, :, :]).reshape(group, 64, width)
    fluid = lax.optimization_barrier(jnp.sum(partial_sum * planes[:, None], axis=2))
    relative = fluid - carried
    speed = jnp.sqrt(lax.optimization_barrier(jnp.sum(relative * relative, axis=1)))
    factor = coefs[:, 0] * (1.0 + 0.15 * jnp.power(coefs[:, 1] * speed, 0.687))
    live = jnp.arange(width, dtype=jnp.int32)[None, :] < filled[:, None]
    drag = jnp.where(live[:, None, :], factor[:, None, :] * relative, jnp.zeros_like(relative))
    weights_s = gauss_rows(position[:, 1], 0.0)
    weights_t = gauss_rows(position[:, 2], 0.0)
    spread = (-drag)[:, :, None, None, :] * weights_s[:, None, :, None, :] * weights_t[:, None, None, :, :]
    spread = spread.reshape(group, 192, width)
    weights_r = jnp.stack([gauss_rows(position[:, 0], 0.0), gauss_rows(position[:, 0], 2.0), gauss_rows(position[:, 0], -2.0)], axis=1)
    deposit = jnp.einsum('gsip,gap->gsia', weights_r, spread, precision=HIGH)
    deposit = deposit.reshape(group, 3, 8, 3, 64).transpose(0, 1, 3, 2, 4).reshape(group, 3, 3, 512)
    return (drag, deposit)

def run_groups(field, position, carried, coefs, filled, group):
    total = field.shape[0]
    turns = total // group
    packed = tuple((a.reshape((turns, group) + a.shape[1:]) for a in (field, position, carried, coefs, filled)))
    drag, deposit = lax.map(lambda args: element_step(*args), packed)
    return (drag.reshape((total,) + drag.shape[2:]), deposit.reshape((total,) + deposit.shape[2:]))

def dss_axis(field, elem_axis, node_axis, far_lo, far_hi):
    count = field.shape[elem_axis]
    lower = lax.slice_in_dim(field, 0, 1, axis=node_axis)
    upper = lax.slice_in_dim(field, 7, 8, axis=node_axis)
    edge_shape = lax.slice_in_dim(lower, 0, 1, axis=elem_axis).shape
    lower_next = jnp.concatenate([lax.slice_in_dim(lower, 1, count, axis=elem_axis), far_lo.reshape(edge_shape)], axis=elem_axis)
    upper_prev = jnp.concatenate([far_hi.reshape(edge_shape), lax.slice_in_dim(upper, 0, count - 1, axis=elem_axis)], axis=elem_axis)
    middle = lax.slice_in_dim(field, 1, 7, axis=node_axis)
    return jnp.concatenate([lower + upper_prev, middle, upper + lower_next], axis=node_axis)

def edge_zeros(field, elem_axis, node_axis):
    edge = lax.slice_in_dim(lax.slice_in_dim(field, 0, 1, axis=elem_axis), 0, 1, axis=node_axis)
    return jnp.zeros_like(edge).reshape(-1)

def reference(velocity, part_pos, part_vel, part_coef, counts, dest, elem):
    blocks = part_pos.shape[0]
    source_row = jnp.arange(blocks, dtype=jnp.int32) // (E_DEV * N_GY)
    local_x = elem // (EYD * EZ)
    local_y = elem // EZ % EYD
    local_z = elem % EZ
    global_id = ((source_row * EXD + local_x) * NEY + dest * EYD + local_y) * EZ + local_z
    by_elem = jnp.argsort(global_id)
    field_e = velocity.reshape(3, blocks, NODES).transpose(1, 0, 2).astype(jnp.float32)
    drag_e, deposit = run_groups(field_e, part_pos[by_elem], part_vel[by_elem], part_coef[by_elem], counts[by_elem], math.gcd(blocks, 256))
    drag = drag_e[global_id]
    deposit = deposit.transpose(1, 2, 0, 3).reshape(3, 3, NEX, NEY, EZ, 8, 8, 8)
    own_part, minus_part, plus_part = (deposit[0], deposit[1], deposit[2])
    empty_layer = jnp.zeros_like(own_part[:, 0:1])
    total = own_part + jnp.concatenate([minus_part[:, 1:], empty_layer], axis=1) + jnp.concatenate([empty_layer, plus_part[:, :-1]], axis=1)
    field = total
    for elem_axis, node_axis in ((1, 4), (2, 5), (3, 6)):
        zeros_edge = edge_zeros(field, elem_axis, node_axis)
        field = dss_axis(field, elem_axis, node_axis, zeros_edge, zeros_edge)
    return (drag, field.reshape(3, NEX, NEY, EZ, NODES))
```

```python
import functools

import jax
import jax.numpy as jnp
from jax import lax
from jax.experimental import pallas as pl
from jax.experimental.pallas import tpu as pltpu
from jax.sharding import PartitionSpec as P

GLL = (
    -1.0,
    -0.8717401485096066,
    -0.5917001814331423,
    -0.2092992179024789,
    0.2092992179024789,
    0.5917001814331423,
    0.8717401485096066,
    1.0,
)
SHARPNESS = 8.0
MESH = pl.DeviceIdType.MESH
F32 = jnp.float32
BF16 = jnp.bfloat16
I32 = jnp.int32
ROW = tuple((i % 2) * 4 + i // 2 for i in range(8))


def norm_consts():
    out = []
    for i in range(8):
        p = 1.0
        for m in range(8):
            if m != i:
                p *= GLL[i] - GLL[m]
        out.append(1.0 / p)
    return out


NORM = norm_consts()


def lagrange_all(x):
    d = [x - q for q in GLL]
    pre = [None] * 8
    suf = [None] * 8
    for i in range(1, 8):
        pre[i] = d[i - 1] if i == 1 else pre[i - 1] * d[i - 1]
    for i in range(6, -1, -1):
        suf[i] = d[i + 1] if i == 6 else suf[i + 1] * d[i + 1]
    out = []
    for i in range(8):
        if i == 0:
            v = suf[0]
        elif i == 7:
            v = pre[7]
        else:
            v = pre[i] * suf[i]
        out.append(v * NORM[i])
    return out


def gauss_all(x):
    return [jnp.exp(-SHARPNESS * (q - x) * (q - x)) for q in GLL]


def split_bf16(x):
    hi = x.astype(BF16)
    lo = (x - hi.astype(F32)).astype(BF16)
    return hi, lo


def rolled(x, by, axis):
    size = x.shape[axis]
    by = by % size
    if by == 0:
        return x
    return pltpu.roll(x, by, axis)


def kernel(
    field, pos, vel, coef, counts, dest, elem,
    drag_out, src_out,
    send, recv, lab_send, lab_recv, perm_v, perm_s, gt_v, fbuf, lag, gau, fluid, drag_s, ret,
    tot, gsend, grecv, ysend, yrecv,
    sm_sem, lab_ss, lab_rs, dat_ss, dat_rs, ret_ss, ret_rs, gm_ss, gm_rs, gp_ss, gp_rs, y_ss, y_rs,
):
    gx = lax.axis_index("gx")
    me = lax.axis_index("gy")
    n_gx = lax.axis_size("gx")
    n_gy = lax.axis_size("gy")
    has_prev = gx > 0
    has_next = gx < n_gx - 1
    has_lo = me > 0
    has_hi = me < n_gy - 1

    bar = pltpu.get_barrier_semaphore()
    for k in (1, 2, 3):
        pl.semaphore_signal(bar, inc=1, device_id={"gy": lax.rem(me + k, 4)}, device_id_type=MESH)

    @pl.when(has_prev)
    def _():
        pl.semaphore_signal(bar, inc=1, device_id={"gx": gx - 1}, device_id_type=MESH)

    @pl.when(has_next)
    def _():
        pl.semaphore_signal(bar, inc=1, device_id={"gx": gx + 1}, device_id_type=MESH)

    sub = lax.broadcasted_iota(I32, (128, 128), 0)
    lane = lax.broadcasted_iota(I32, (128, 128), 1)
    d_row = dest[...]
    d_b = jnp.broadcast_to(d_row, (128, 128))
    d_t = d_b.T
    before = jnp.where((d_b == d_t) & (sub < lane), 1, 0)
    rank = jnp.sum(before, axis=0, keepdims=True)
    place = d_row * 32 + rank
    p_t = jnp.broadcast_to(place, (128, 128)).T
    e_t = jnp.broadcast_to(elem[...], (128, 128)).T
    perm_v[0:1, :] = jnp.max(jnp.where(p_t == lane, sub, 0), axis=0, keepdims=True)
    perm_v[1:2, :] = d_row * 96 + rank
    to_smem = pltpu.make_async_copy(perm_v, perm_s, sm_sem.at[0])
    to_smem.start()
    mine = (lane >= me * 32) & (lane < me * 32 + 32)
    for k in range(4):
        d = lax.rem(me + k, 4)
        target = lane + (d - me) * 32
        row = jnp.max(jnp.where((p_t == target) & mine, e_t, 0), axis=0, keepdims=True)
        if k == 0:
            lab_recv[me] = row
        else:
            lab_send[k] = row

    pl.semaphore_wait(bar, 3 + (gx + n_gx - 1) // n_gx + (2 * n_gx - 2 - gx) // n_gx)

    def lab_copy(k):
        return pltpu.make_async_remote_copy(
            src_ref=lab_send.at[k], dst_ref=lab_recv.at[me],
            send_sem=lab_ss.at[k], recv_sem=lab_rs.at[lax.rem(4 - k, 4)],
            device_id={"gy": lax.rem(me + k, 4)}, device_id_type=MESH)

    def dat_copy(k):
        return pltpu.make_async_remote_copy(
            src_ref=send.at[k], dst_ref=recv.at[me],
            send_sem=dat_ss.at[k], recv_sem=dat_rs.at[lax.rem(4 - k, 4)],
            device_id={"gy": lax.rem(me + k, 4)}, device_id_type=MESH)

    def ret_copy(k):
        s = lax.rem(me + k, 4)
        return pltpu.make_async_remote_copy(
            src_ref=drag_s.at[pl.ds(pl.multiple_of(s * 96, 96), 96)],
            dst_ref=ret.at[pl.ds(pl.multiple_of(me * 96, 96), 96)],
            send_sem=ret_ss.at[k], recv_sem=ret_rs.at[lax.rem(4 - k, 4)],
            device_id={"gy": s}, device_id_type=MESH)

    for k in (2, 1, 3):
        lab_copy(k).start()
    to_smem.wait()

    slot_lane = lax.broadcasted_iota(I32, (1, 128), 1)

    def pack(dst, at, d):
        def step(g, _):
            for u in range(8):
                m = g * 8 + u
                b = perm_s[0, d * 32 + m]
                live = slot_lane < counts[b]
                c2 = coef[b]
                for c in range(3):
                    dst[at, pl.ds(c * 32 + m, 1), :] = pos[c, pl.ds(b, 1), :]
                    dst[at, pl.ds(96 + c * 32 + m, 1), :] = vel[c, pl.ds(b, 1), :]
                dst[at, pl.ds(192 + m, 1), :] = jnp.where(live, c2[0:1], 0.0)
                dst[at, pl.ds(224 + m, 1), :] = c2[1:2]
            return 0

        lax.fori_loop(0, 4, step, 0)

    def pack_and_send(q, _):
        k = 2 - q + 3 * (q // 2)
        pack(send, k, lax.rem(me + k, 4))
        dat_copy(k).start()
        return 0

    lax.fori_loop(0, 3, pack_and_send, 0)
    pack(recv, me, me)

    half = lax.broadcasted_iota(I32, (16, 128), 1) < 64

    def spread_field(n, _):
        c = n // 8
        ex = lax.rem(n // 4, 2)
        ey = lax.rem(n, 4)
        base = (ex * 4 + ey) * 16 * 24 + c * 8
        for t in range(4):
            x = field[c, ex, ey, :, t * 128:(t + 1) * 128].astype(F32)
            y = pltpu.roll(x, 64, 1)
            fbuf[pl.ds(base + t, 16, stride=24), :] = jnp.where(half, x, y)
            fbuf[pl.ds(base + 4 + t, 16, stride=24), :] = jnp.where(half, y, x)
        return 0

    lax.fori_loop(0, 24, spread_field, 0)

    for k in (1, 3, 2):
        lab_copy(k).wait()
    labels = lab_recv[0] + lab_recv[1] + lab_recv[2] + lab_recv[3]
    g_t = jnp.broadcast_to(labels, (128, 128)).T
    gt_v[...] = g_t
    inv = jnp.max(jnp.where(g_t == lane, sub, 0), axis=0, keepdims=True)
    perm_v[2:3, :] = labels
    perm_v[3:4, :] = inv
    perm_v[4:5, :] = (inv // 32) * 96 + lax.rem(inv, 32)
    to_smem = pltpu.make_async_copy(perm_v, perm_s, sm_sem.at[0])
    to_smem.start()
    to_smem.wait()

    hp = jnp.where(has_prev, 1.0, 0.0).astype(F32)
    hn = jnp.where(has_next, 1.0, 0.0).astype(F32)

    def chunk(q, _):
        k = lax.rem((q * q + q) // 2, 4)
        s = lax.rem(me + k, 4)

        @pl.when(q > 0)
        def _():
            dat_copy(lax.rem(4 - k, 4)).wait_recv()

        def bulk(g, _):
            first = s * 32 + g * 8

            def rows_of(r):
                return recv[s, pl.ds(pl.multiple_of(r * 32 + g * 8, 8), 8), :]

            def put(ref, kind, row, v):
                ref[kind, pl.ds(first * 8 + row, 8, stride=8), :] = v

            r, sc, tc = rows_of(0), rows_of(1), rows_of(2)
            lr, ls, lt = lagrange_all(r), lagrange_all(sc), lagrange_all(tc)
            for i in range(8):
                put(lag, 0, ROW[i], lr[i])
                put(lag, 1, i, ls[i])
                put(lag, 2, i, lt[i])
            ex0 = gt_v[pl.ds(pl.multiple_of(first, 8), 8), :] < 64
            own, minus, plus = gauss_all(r), gauss_all(r + 2.0), gauss_all(r - 2.0)
            zero = jnp.zeros_like(r)
            for i in range(8):
                o, p, m, x = own[i], plus[i], minus[i], zero
                if i == 0:
                    o = o + jnp.where(ex0, hp * minus[7], minus[7])
                    p = p + own[7]
                    x = jnp.where(ex0, plus[7], 0.0)
                if i == 7:
                    o = o + jnp.where(ex0, plus[0], hn * plus[0])
                    m = m + own[0]
                    x = jnp.where(ex0, 0.0, minus[0])
                put(gau, 0, ROW[i], o)
                put(gau, 1, ROW[i], p)
                put(gau, 2, ROW[i], m)
                put(gau, 3, ROW[i], x)
            gs, gt = gauss_all(sc), gauss_all(tc)
            for i in range(8):
                put(gau, 4, i, gs[i])
                put(gau, 5, i, gt[i])
            return 0

        lax.fori_loop(0, 4, bulk, 0)

        def interp(g, _):
            for u in range(4):
                slot = s * 32 + g * 4 + u
                e = perm_s[2, slot]
                f = fbuf[pl.ds(e * 24, 24), :].astype(BF16)
                at = pl.multiple_of(slot * 8, 8)
                lt = lag[2, pl.ds(at, 8), :]
                ls = lag[1, pl.ds(at, 8), :]
                plane = jnp.concatenate([ls[j:j + 1] * lt for j in range(8)], axis=0)
                hi, lo = split_bf16(plane)
                out = jnp.dot(f, jnp.concatenate([hi, lo], axis=0), preferred_element_type=F32)
                lr = lag[0, pl.ds(at, 8), :]
                for c in range(3):
                    fluid[c, pl.ds(slot, 1), :] = jnp.sum(out[8 * c:8 * c + 8] * lr, axis=0, keepdims=True)
            return 0

        lax.fori_loop(0, 8, interp, 0)

        rel = []
        for c in range(3):
            rel.append(fluid[c, pl.ds(pl.multiple_of(s * 32, 32), 32), :]
                       - recv[s, 96 + c * 32:128 + c * 32, :])
        speed = jnp.sqrt(rel[0] * rel[0] + rel[1] * rel[1] + rel[2] * rel[2])
        reynolds = jnp.maximum(recv[s, 224:256, :] * speed, 1e-30)
        factor = recv[s, 192:224, :] * (1.0 + 0.15 * jnp.exp(0.687 * jnp.log(reynolds)))
        for c in range(3):
            drag_s[pl.ds(pl.multiple_of(s * 96 + c * 32, 32), 32), :] = factor * rel[c]

        @pl.when(q > 0)
        def _():
            ret_copy(k).start()
        return 0

    lax.fori_loop(0, 4, chunk, 0)
    own_rows = pl.ds(pl.multiple_of(me * 96, 96), 96)
    ret[own_rows, :] = drag_s[own_rows, :]

    half8 = lax.broadcasted_iota(I32, (8, 128), 1) < 64

    def gm_copy(ey):
        return pltpu.make_async_remote_copy(
            src_ref=gsend.at[0, ey], dst_ref=grecv.at[0, ey], send_sem=gm_ss.at[ey], recv_sem=gm_rs.at[ey],
            device_id={"gx": gx - 1}, device_id_type=MESH)

    def gp_copy(ey):
        return pltpu.make_async_remote_copy(
            src_ref=gsend.at[1, ey], dst_ref=grecv.at[1, ey], send_sem=gp_ss.at[ey], recv_sem=gp_rs.at[ey],
            device_id={"gx": gx + 1}, device_id_type=MESH)

    def weights(slot, drow, order):
        at = slot * 8
        gs = gau[4, pl.ds(at, 8), :]
        gt = gau[5, pl.ds(at, 8), :]
        plane = jnp.concatenate([gs[j:j + 1] * gt for j in range(8)], axis=0)
        hi, lo = split_bf16(plane)
        rhs = jnp.concatenate([hi, lo], axis=0)
        d = [jnp.broadcast_to(-drag_s[pl.ds(drow + c * 32, 1), :], (8, 128)) for c in range(3)]
        w = [gau[n, pl.ds(at, 8), :] for n in order]
        lhs = jnp.concatenate([a * d[c] for a in w for c in range(3)], axis=0)
        lhi, llo = split_bf16(lhs)
        return rhs, lhi, llo

    def deposit_row(q, _):
        ey = lax.rem(3 * q, 4)

        def pair_group(g, _):
            for u in range(2):
                ez = g * 2 + u
                e0 = ey * 16 + ez
                e1 = 64 + e0
                r0, h0, l0 = weights(perm_s[3, e0], perm_s[4, e0], (0, 1, 2, 3))
                r1, h1, l1 = weights(perm_s[3, e1], perm_s[4, e1], (2, 0, 3, 1))
                lhs = jnp.concatenate(
                    [jnp.concatenate([h0, h1], axis=1), jnp.concatenate([l0, l1], axis=1)], axis=0)
                rhs = jnp.concatenate([r0, r1], axis=1)
                out = lax.dot_general(lhs, rhs, (((1,), (1,)), ((), ())), preferred_element_type=F32)
                z = out[0:96] + out[96:192]
                z = z + pltpu.roll(z, 64, 1)
                ezh = ez // 8
                ezl = lax.rem(ez, 8)
                for o in range(4):
                    for c in range(3):
                        v = z[(o * 3 + c) * 8:(o * 3 + c) * 8 + 8]
                        v = jnp.where(half8, v, pltpu.roll(v, 4, 0))[0:4]
                        if o < 2:
                            tot[c, o, ey, pl.ds(ezh * 32 + ezl, 4, stride=8), :] = v
                        else:
                            gsend[o - 2, ey, c, pl.ds(ezh * 32 + ezl, 4, stride=8), :] = v
            return 0

        lax.fori_loop(0, 8, pair_group, 0)

        @pl.when(has_prev)
        def _():
            gm_copy(ey).start()

        @pl.when(has_next)
        def _():
            gp_copy(ey).start()
        return 0

    lax.fori_loop(0, 4, deposit_row, 0)

    for k in (1, 3, 2):
        ret_copy(k).wait()

    def unpack(g, _):
        for u in range(8):
            b = g * 8 + u
            row = perm_s[1, b]
            for c in range(3):
                drag_out[c, pl.ds(b, 1), :] = ret[pl.ds(row + c * 32, 1), :]
        return 0

    lax.fori_loop(0, 16, unpack, 0)

    half32 = lax.broadcasted_iota(I32, (8, 128), 1) < 64

    def add_ghost(q, _):
        ey = lax.rem(3 * q, 4)

        @pl.when(has_next)
        def _():
            gm_copy(ey).wait_recv()

        @pl.when(jnp.logical_not(has_next))
        def _():
            grecv[0, ey] = jnp.zeros((3, 64, 128), F32)

        @pl.when(has_prev)
        def _():
            gp_copy(ey).wait_recv()

        @pl.when(jnp.logical_not(has_prev))
        def _():
            grecv[1, ey] = jnp.zeros((3, 64, 128), F32)

        for c in range(3):
            for h in range(2):
                for t in range(4):
                    rows = slice(h * 32 + t * 8, h * 32 + t * 8 + 8)
                    up = grecv[0, ey, c, rows, :]
                    down = grecv[1, ey, c, rows, :]
                    if t == 0:
                        far = pltpu.roll(grecv[1, ey, c, h * 32 + 24:h * 32 + 32, :], 64, 1)
                        up = up + jnp.where(half32, far, 0.0)
                    if t == 3:
                        far = pltpu.roll(grecv[0, ey, c, h * 32:h * 32 + 8, :], 64, 1)
                        down = down + jnp.where(half32, 0.0, far)
                    tot[c, 0, ey, rows, :] = tot[c, 0, ey, rows, :] + down
                    tot[c, 1, ey, rows, :] = tot[c, 1, ey, rows, :] + up
        return 0

    lax.fori_loop(0, 2, add_ghost, 0)

    lane8 = lax.broadcasted_iota(I32, (8, 128), 1)
    j8 = lax.rem(lane8 // 8, 8)
    for c in range(3):
        for h in range(2):
            lo_face = jnp.zeros((8, 128), F32)
            hi_face = jnp.zeros((8, 128), F32)
            for ex in range(2):
                for t in range(4):
                    n = ex * 4 + t
                    rows = slice(h * 32 + t * 8, h * 32 + t * 8 + 8)
                    lo_face = jnp.where(j8 == n, rolled(tot[c, ex, 0, rows, :], 8 * n, 1), lo_face)
                    hi_face = jnp.where(j8 == n, rolled(tot[c, ex, 3, rows, :], 8 * n - 56, 1), hi_face)
            ysend[0, (c * 2 + h) * 8:(c * 2 + h) * 8 + 8, :] = lo_face
            ysend[1, (c * 2 + h) * 8:(c * 2 + h) * 8 + 8, :] = hi_face

    def y_copy(way):
        return pltpu.make_async_remote_copy(
            src_ref=ysend.at[way], dst_ref=yrecv.at[way], send_sem=y_ss.at[way], recv_sem=y_rs.at[way],
            device_id={"gy": me - 1 if way == 0 else me + 1}, device_id_type=MESH)

    @pl.when(has_lo)
    def _():
        y_copy(0).start()

    @pl.when(has_hi)
    def _():
        y_copy(1).start()

    lax.fori_loop(2, 4, add_ghost, 0)

    @pl.when(has_hi)
    def _():
        y_copy(0).wait_recv()

    @pl.when(jnp.logical_not(has_hi))
    def _():
        yrecv[0] = jnp.zeros((48, 128), F32)

    @pl.when(has_lo)
    def _():
        y_copy(1).wait_recv()

    @pl.when(jnp.logical_not(has_lo))
    def _():
        yrecv[1] = jnp.zeros((48, 128), F32)

    lane16 = lax.broadcasted_iota(I32, (16, 128), 1)
    row16 = lax.broadcasted_iota(I32, (16, 128), 0)
    j16 = lax.rem(lane16 // 8, 8)
    k16 = lax.rem(lane16, 8)
    z_up = (k16 == 7) & (row16 < 15)
    z_down = (k16 == 0) & (row16 > 0)

    def finish(c, _):
        for ex in range(2):
            for t in range(4):
                n = ex * 4 + t
                lo_rows = slice(t * 8, t * 8 + 8)
                hi_rows = slice(32 + t * 8, 32 + t * 8 + 8)
                x = [jnp.concatenate([tot[c, ex, ey, lo_rows, :], tot[c, ex, ey, hi_rows, :]], axis=0)
                     for ey in range(4)]
                face = pl.ds(pl.multiple_of(c * 16, 16), 16)
                from_hi = rolled(yrecv[0, face, :], 56 - 8 * n, 1)
                from_lo = rolled(yrecv[1, face, :], -8 * n, 1)
                for ey in range(4):
                    nxt = from_hi if ey == 3 else pltpu.roll(x[ey + 1], 56, 1)
                    prv = from_lo if ey == 0 else pltpu.roll(x[ey - 1], 72, 1)
                    y = x[ey] + jnp.where(j16 == 7, nxt, jnp.where(j16 == 0, prv, 0.0))
                    above = pltpu.roll(pltpu.roll(y, 7, 1), 15, 0)
                    below = pltpu.roll(pltpu.roll(y, 121, 1), 1, 0)
                    src_out[c, ex, ey, :, t * 128:(t + 1) * 128] = y + jnp.where(
                        z_up, above, jnp.where(z_down, below, 0.0))
        return 0

    lax.fori_loop(0, 3, finish, 0)

    for k in (1, 2, 3):
        dat_copy(k).wait_send()

    for ey in range(4):
        @pl.when(has_prev)
        def _():
            gm_copy(ey).wait_send()

        @pl.when(has_next)
        def _():
            gp_copy(ey).wait_send()

    @pl.when(has_lo)
    def _():
        y_copy(0).wait_send()

    @pl.when(has_hi)
    def _():
        y_copy(1).wait_send()


def body(velocity, part_pos, part_vel, part_coef, counts, dest, elem):
    vm = pl.BlockSpec(memory_space=pltpu.VMEM)
    sm = pl.BlockSpec(memory_space=pltpu.SMEM)
    dma = pltpu.SemaphoreType.DMA
    drag, source = pl.pallas_call(
        kernel,
        out_shape=(
            jax.ShapeDtypeStruct((3, 128, 128), F32),
            jax.ShapeDtypeStruct(velocity.shape, F32),
        ),
        in_specs=[vm, vm, vm, vm, sm, vm, vm],
        out_specs=(vm, vm),
        scratch_shapes=[
            pltpu.VMEM((4, 256, 128), F32),
            pltpu.VMEM((4, 256, 128), F32),
            pltpu.VMEM((4, 1, 128), I32),
            pltpu.VMEM((4, 1, 128), I32),
            pltpu.VMEM((8, 128), I32),
            pltpu.SMEM((8, 128), I32),
            pltpu.VMEM((128, 128), I32),
            pltpu.VMEM((3072, 128), F32),
            pltpu.VMEM((3, 1024, 128), F32),
            pltpu.VMEM((6, 1024, 128), F32),
            pltpu.VMEM((3, 128, 128), F32),
            pltpu.VMEM((384, 128), F32),
            pltpu.VMEM((384, 128), F32),
            pltpu.VMEM((3, 2, 4, 64, 128), F32),
            pltpu.VMEM((2, 4, 3, 64, 128), F32),
            pltpu.VMEM((2, 4, 3, 64, 128), F32),
            pltpu.VMEM((2, 48, 128), F32),
            pltpu.VMEM((2, 48, 128), F32),
            dma((1,)), dma((4,)), dma((4,)), dma((4,)), dma((4,)), dma((4,)), dma((4,)),
            dma((4,)), dma((4,)), dma((4,)), dma((4,)), dma((2,)), dma((2,)),
        ],
        compiler_params=pltpu.CompilerParams(
            collective_id=0, has_side_effects=True, vmem_limit_bytes=40 * 1024 * 1024),
    )(velocity, part_pos.transpose(1, 0, 2), part_vel.transpose(1, 0, 2), part_coef, counts,
      dest.reshape(1, 128), elem.reshape(1, 128))
    return drag.transpose(1, 0, 2), source


def solution(mesh):
    in_specs = (
        P(None, "gx", "gy", None, None),
        P(("gx", "gy"), None, None),
        P(("gx", "gy"), None, None),
        P(("gx", "gy"), None, None),
        P(("gx", "gy")),
        P(("gx", "gy")),
        P(("gx", "gy")),
    )
    out_specs = (P(("gx", "gy"), None, None), P(None, "gx", "gy", None, None))
    return jax.shard_map(body, mesh=mesh, in_specs=in_specs, out_specs=out_specs, check_vma=False)
```

```python
import functools

import jax
import jax.numpy as jnp
from jax import lax
from jax.experimental import pallas as pl
from jax.experimental.pallas import tpu as pltpu
from jax.sharding import PartitionSpec as P

GLL = (
    -1.0,
    -0.8717401485096066,
    -0.5917001814331423,
    -0.2092992179024789,
    0.2092992179024789,
    0.5917001814331423,
    0.8717401485096066,
    1.0,
)
SHARPNESS = 8.0
MESH = pl.DeviceIdType.MESH
F32 = jnp.float32
BF16 = jnp.bfloat16
I32 = jnp.int32
ROW = tuple((i % 2) * 4 + i // 2 for i in range(8))


def norm_consts():
    out = []
    for i in range(8):
        p = 1.0
        for m in range(8):
            if m != i:
                p *= GLL[i] - GLL[m]
        out.append(1.0 / p)
    return out


NORM = norm_consts()


def lagrange_all(x):
    d = [x - q for q in GLL]
    pre = [None] * 8
    suf = [None] * 8
    for i in range(1, 8):
        pre[i] = d[i - 1] if i == 1 else pre[i - 1] * d[i - 1]
    for i in range(6, -1, -1):
        suf[i] = d[i + 1] if i == 6 else suf[i + 1] * d[i + 1]
    out = []
    for i in range(8):
        if i == 0:
            v = suf[0]
        elif i == 7:
            v = pre[7]
        else:
            v = pre[i] * suf[i]
        out.append(v * NORM[i])
    return out


def gauss_all(x):
    return [jnp.exp(-SHARPNESS * (q - x) * (q - x)) for q in GLL]


def split_bf16(x):
    hi = x.astype(BF16)
    lo = (x - hi.astype(F32)).astype(BF16)
    return hi, lo


def rolled(x, by, axis):
    size = x.shape[axis]
    by = by % size
    if by == 0:
        return x
    return pltpu.roll(x, by, axis)


def kernel(
    field_h, pos_h, vel_h, coef_h, counts_h, dest_h, elem_h,
    drag_out, src_out,
    field, pos, vel, coef, counts, dest, elem, in_sem,
    send, recv, lab_send, lab_recv, perm_v, perm_s, gt_v, fbuf, lag, gau, fluid, drag_s, ret,
    tot, ztot, gsend, grecv, ysend, yrecv,
    sm_sem, lab_ss, lab_rs, dat_ss, dat_rs, ret_ss, ret_rs, gm_ss, gm_rs, gp_ss, gp_rs, y_ss, y_rs,
):
    gx = lax.axis_index("gx")
    me = lax.axis_index("gy")
    n_gx = lax.axis_size("gx")
    n_gy = lax.axis_size("gy")
    has_prev = gx > 0
    has_next = gx < n_gx - 1
    has_lo = me > 0
    has_hi = me < n_gy - 1

    ins = [
        pltpu.make_async_copy(a, b, in_sem.at[n])
        for n, (a, b) in enumerate((
            (dest_h, dest), (elem_h, elem), (counts_h, counts), (pos_h, pos), (vel_h, vel), (coef_h, coef),
            (field_h, field)))
    ]
    for copy in ins:
        copy.start()

    bar = pltpu.get_barrier_semaphore()
    for k in (1, 2, 3):
        pl.semaphore_signal(bar, inc=1, device_id={"gy": lax.rem(me + k, 4)}, device_id_type=MESH)

    @pl.when(has_prev)
    def _():
        pl.semaphore_signal(bar, inc=1, device_id={"gx": gx - 1}, device_id_type=MESH)

    @pl.when(has_next)
    def _():
        pl.semaphore_signal(bar, inc=1, device_id={"gx": gx + 1}, device_id_type=MESH)

    sub = lax.broadcasted_iota(I32, (128, 128), 0)
    lane = lax.broadcasted_iota(I32, (128, 128), 1)
    ins[0].wait()
    ins[1].wait()
    d_row = dest[...]
    d_b = jnp.broadcast_to(d_row, (128, 128))
    d_t = d_b.T
    before = jnp.where((d_b == d_t) & (sub < lane), 1, 0)
    rank = jnp.sum(before, axis=0, keepdims=True)
    place = d_row * 32 + rank
    p_t = jnp.broadcast_to(place, (128, 128)).T
    e_t = jnp.broadcast_to(elem[...], (128, 128)).T
    perm_v[0:1, :] = jnp.max(jnp.where(p_t == lane, sub, 0), axis=0, keepdims=True)
    perm_v[1:2, :] = d_row * 96 + rank
    to_smem = pltpu.make_async_copy(perm_v, perm_s, sm_sem.at[0])
    to_smem.start()
    mine = (lane >= me * 32) & (lane < me * 32 + 32)
    for k in range(4):
        d = lax.rem(me + k, 4)
        target = lane + (d - me) * 32
        row = jnp.max(jnp.where((p_t == target) & mine, e_t, 0), axis=0, keepdims=True)
        if k == 0:
            lab_recv[me] = row
        else:
            lab_send[k] = row

    pl.semaphore_wait(bar, 3 + (gx + n_gx - 1) // n_gx + (2 * n_gx - 2 - gx) // n_gx)

    def lab_copy(k):
        return pltpu.make_async_remote_copy(
            src_ref=lab_send.at[k], dst_ref=lab_recv.at[me],
            send_sem=lab_ss.at[k], recv_sem=lab_rs.at[lax.rem(4 - k, 4)],
            device_id={"gy": lax.rem(me + k, 4)}, device_id_type=MESH)

    def dat_copy(k):
        return pltpu.make_async_remote_copy(
            src_ref=send.at[k], dst_ref=recv.at[me],
            send_sem=dat_ss.at[k], recv_sem=dat_rs.at[lax.rem(4 - k, 4)],
            device_id={"gy": lax.rem(me + k, 4)}, device_id_type=MESH)

    def ret_copy(k):
        s = lax.rem(me + k, 4)
        return pltpu.make_async_remote_copy(
            src_ref=drag_s.at[pl.ds(pl.multiple_of(s * 96, 96), 96)],
            dst_ref=ret.at[pl.ds(pl.multiple_of(me * 96, 96), 96)],
            send_sem=ret_ss.at[k], recv_sem=ret_rs.at[lax.rem(4 - k, 4)],
            device_id={"gy": s}, device_id_type=MESH)

    for k in (2, 1, 3):
        lab_copy(k).start()
    to_smem.wait()

    slot_lane = lax.broadcasted_iota(I32, (1, 128), 1)

    def pack(dst, at, d):
        def step(g, _):
            for u in range(8):
                m = g * 8 + u
                b = perm_s[0, d * 32 + m]
                live = slot_lane < counts[b]
                c2 = coef[b]
                for c in range(3):
                    dst[at, pl.ds(c * 32 + m, 1), :] = pos[c, pl.ds(b, 1), :]
                    dst[at, pl.ds(96 + c * 32 + m, 1), :] = vel[c, pl.ds(b, 1), :]
                dst[at, pl.ds(192 + m, 1), :] = jnp.where(live, c2[0:1], 0.0)
                dst[at, pl.ds(224 + m, 1), :] = c2[1:2]
            return 0

        lax.fori_loop(0, 4, step, 0)

    for n in (2, 3, 4, 5):
        ins[n].wait()

    def pack_and_send(q, _):
        k = 2 - q + 3 * (q // 2)
        pack(send, k, lax.rem(me + k, 4))
        dat_copy(k).start()
        return 0

    lax.fori_loop(0, 3, pack_and_send, 0)
    pack(recv, me, me)

    half = lax.broadcasted_iota(I32, (16, 128), 1) < 64

    ins[6].wait()

    def spread_field(n, _):
        c = n // 8
        ex = lax.rem(n // 4, 2)
        ey = lax.rem(n, 4)
        base = (ex * 4 + ey) * 16 * 24 + c * 8
        for t in range(4):
            x = field[c, ex, ey, :, t * 128:(t + 1) * 128].astype(F32)
            y = pltpu.roll(x, 64, 1)
            fbuf[pl.ds(base + t, 16, stride=24), :] = jnp.where(half, x, y)
            fbuf[pl.ds(base + 4 + t, 16, stride=24), :] = jnp.where(half, y, x)
        return 0

    lax.fori_loop(0, 24, spread_field, 0)

    for k in (1, 3, 2):
        lab_copy(k).wait()
    labels = lab_recv[0] + lab_recv[1] + lab_recv[2] + lab_recv[3]
    g_t = jnp.broadcast_to(labels, (128, 128)).T
    gt_v[...] = g_t
    inv = jnp.max(jnp.where(g_t == lane, sub, 0), axis=0, keepdims=True)
    perm_v[2:3, :] = labels
    perm_v[3:4, :] = inv
    perm_v[4:5, :] = (inv // 32) * 96 + lax.rem(inv, 32)
    to_smem = pltpu.make_async_copy(perm_v, perm_s, sm_sem.at[0])
    to_smem.start()
    to_smem.wait()

    hp = jnp.where(has_prev, 1.0, 0.0).astype(F32)
    hn = jnp.where(has_next, 1.0, 0.0).astype(F32)

    def chunk(q, _):
        k = lax.rem((q * q + q) // 2, 4)
        s = lax.rem(me + k, 4)

        @pl.when(q > 0)
        def _():
            dat_copy(lax.rem(4 - k, 4)).wait_recv()

        def bulk(g, _):
            first = s * 32 + g * 8

            def rows_of(r):
                return recv[s, pl.ds(pl.multiple_of(r * 32 + g * 8, 8), 8), :]

            def put(ref, kind, row, v):
                ref[kind, pl.ds(first * 8 + row, 8, stride=8), :] = v

            r, sc, tc = rows_of(0), rows_of(1), rows_of(2)
            lr, ls, lt = lagrange_all(r), lagrange_all(sc), lagrange_all(tc)
            for i in range(8):
                put(lag, 0, ROW[i], lr[i])
                put(lag, 1, i, ls[i])
                put(lag, 2, i, lt[i])
            ex0 = gt_v[pl.ds(pl.multiple_of(first, 8), 8), :] < 64
            own, minus, plus = gauss_all(r), gauss_all(r + 2.0), gauss_all(r - 2.0)
            zero = jnp.zeros_like(r)
            for i in range(8):
                o, p, m, x = own[i], plus[i], minus[i], zero
                if i == 0:
                    o = o + jnp.where(ex0, hp * minus[7], minus[7])
                    p = p + own[7]
                    x = jnp.where(ex0, plus[7], 0.0)
                if i == 7:
                    o = o + jnp.where(ex0, plus[0], hn * plus[0])
                    m = m + own[0]
                    x = jnp.where(ex0, 0.0, minus[0])
                put(gau, 0, ROW[i], o)
                put(gau, 1, ROW[i], p)
                put(gau, 2, ROW[i], m)
                put(gau, 3, ROW[i], x)
            gs, gt = gauss_all(sc), gauss_all(tc)
            for i in range(8):
                put(gau, 4, i, gs[i])
                put(gau, 5, i, gt[i])
            return 0

        lax.fori_loop(0, 4, bulk, 0)

        def interp(g, _):
            for u in range(32):
                slot = s * 32 + g * 32 + u
                e = perm_s[2, slot]
                f = fbuf[pl.ds(e * 24, 24), :].astype(BF16)
                at = pl.multiple_of(slot * 8, 8)
                lt = lag[2, pl.ds(at, 8), :]
                ls = lag[1, pl.ds(at, 8), :]
                plane = jnp.concatenate([ls[j:j + 1] * lt for j in range(8)], axis=0)
                hi, lo = split_bf16(plane)
                out = jnp.dot(f, jnp.concatenate([hi, lo], axis=0), preferred_element_type=F32)
                lr = lag[0, pl.ds(at, 8), :]
                for c in range(3):
                    fluid[c, pl.ds(slot, 1), :] = jnp.sum(out[8 * c:8 * c + 8] * lr, axis=0, keepdims=True)
            return 0

        interp(0, 0)

        rel = []
        for c in range(3):
            rel.append(fluid[c, pl.ds(pl.multiple_of(s * 32, 32), 32), :]
                       - recv[s, 96 + c * 32:128 + c * 32, :])
        speed = jnp.sqrt(rel[0] * rel[0] + rel[1] * rel[1] + rel[2] * rel[2])
        reynolds = jnp.maximum(recv[s, 224:256, :] * speed, 1e-30)
        factor = recv[s, 192:224, :] * (1.0 + 0.15 * jnp.exp(0.687 * jnp.log(reynolds)))
        for c in range(3):
            drag_s[pl.ds(pl.multiple_of(s * 96 + c * 32, 32), 32), :] = factor * rel[c]

        @pl.when(q > 0)
        def _():
            ret_copy(k).start()
        return 0

    lax.fori_loop(0, 4, chunk, 0)
    own_rows = pl.ds(pl.multiple_of(me * 96, 96), 96)
    ret[own_rows, :] = drag_s[own_rows, :]

    half8 = lax.broadcasted_iota(I32, (8, 128), 1) < 64

    def gm_copy(ey):
        return pltpu.make_async_remote_copy(
            src_ref=gsend.at[0, ey], dst_ref=grecv.at[0, ey], send_sem=gm_ss.at[ey], recv_sem=gm_rs.at[ey],
            device_id={"gx": gx - 1}, device_id_type=MESH)

    def gp_copy(ey):
        return pltpu.make_async_remote_copy(
            src_ref=gsend.at[1, ey], dst_ref=grecv.at[1, ey], send_sem=gp_ss.at[ey], recv_sem=gp_rs.at[ey],
            device_id={"gx": gx + 1}, device_id_type=MESH)

    def weights(slot, drow, order):
        at = slot * 8
        gs = gau[4, pl.ds(at, 8), :]
        gt = gau[5, pl.ds(at, 8), :]
        plane = jnp.concatenate([gs[j:j + 1] * gt for j in range(8)], axis=0)
        hi, lo = split_bf16(plane)
        rhs = jnp.concatenate([hi, lo], axis=0)
        d = [jnp.broadcast_to(-drag_s[pl.ds(drow + c * 32, 1), :], (8, 128)) for c in range(3)]
        w = [gau[n, pl.ds(at, 8), :] for n in order]
        lhs = jnp.concatenate([a * d[c] for a in w for c in range(3)], axis=0)
        lhi, llo = split_bf16(lhs)
        return rhs, lhi, llo

    def deposit_row(q, _):
        ey = lax.rem(3 * q, 4)

        def pair_group(g, _):
            for u in range(16):
                ez = g * 16 + u
                e0 = ey * 16 + ez
                e1 = 64 + e0
                r0, h0, l0 = weights(perm_s[3, e0], perm_s[4, e0], (0, 1, 2, 3))
                r1, h1, l1 = weights(perm_s[3, e1], perm_s[4, e1], (2, 0, 3, 1))
                lhs = jnp.concatenate(
                    [jnp.concatenate([h0, h1], axis=1), jnp.concatenate([l0, l1], axis=1)], axis=0)
                rhs = jnp.concatenate([r0, r1], axis=1)
                out = lax.dot_general(lhs, rhs, (((1,), (1,)), ((), ())), preferred_element_type=F32)
                z = out[0:96] + out[96:192]
                z = z + pltpu.roll(z, 64, 1)
                ezh, ezl = ez // 8, ez % 8
                for o in range(4):
                    for c in range(3):
                        v = z[(o * 3 + c) * 8:(o * 3 + c) * 8 + 8]
                        v = jnp.where(half8, v, pltpu.roll(v, 4, 0))[0:4]
                        if o < 2:
                            tot[c, o, ey, pl.ds(ezh * 32 + ezl, 4, stride=8), :] = v
                        else:
                            gsend[o - 2, ey, c, pl.ds(ezh * 32 + ezl, 4, stride=8), :] = v
            return 0

        pair_group(0, 0)

        @pl.when(has_prev)
        def _():
            gm_copy(ey).start()

        @pl.when(has_next)
        def _():
            gp_copy(ey).start()
        return 0

    lax.fori_loop(0, 4, deposit_row, 0)

    for k in (1, 3, 2):
        ret_copy(k).wait()

    def unpack(g, _):
        for u in range(8):
            b = g * 8 + u
            row = perm_s[1, b]
            for c in range(3):
                drag_out[c, pl.ds(b, 1), :] = ret[pl.ds(row + c * 32, 1), :]
        return 0

    lax.fori_loop(0, 16, unpack, 0)

    lane16 = lax.broadcasted_iota(I32, (16, 128), 1)
    row16 = lax.broadcasted_iota(I32, (16, 128), 0)
    j16 = lax.rem(lane16 // 8, 8)
    half16 = lane16 < 64
    k16 = lax.rem(lane16, 8)
    z_up = (k16 == 7) & (row16 < 15)
    z_down = (k16 == 0) & (row16 > 0)

    def add_ghost(q, _):
        ey = lax.rem(3 * q, 4)

        @pl.when(has_next)
        def _():
            gm_copy(ey).wait_recv()

        @pl.when(jnp.logical_not(has_next))
        def _():
            grecv[0, ey] = jnp.zeros((3, 64, 128), F32)

        @pl.when(has_prev)
        def _():
            gp_copy(ey).wait_recv()

        @pl.when(jnp.logical_not(has_prev))
        def _():
            grecv[1, ey] = jnp.zeros((3, 64, 128), F32)

        def tile(ref, t):
            return jnp.concatenate([ref[t * 8:t * 8 + 8, :], ref[32 + t * 8:40 + t * 8, :]], axis=0)

        for c in range(3):
            for t in range(4):
                up = tile(grecv.at[0, ey, c], t)
                down = tile(grecv.at[1, ey, c], t)
                if t == 0:
                    up = up + jnp.where(half16, pltpu.roll(tile(grecv.at[1, ey, c], 3), 64, 1), 0.0)
                if t == 3:
                    down = down + jnp.where(half16, 0.0, pltpu.roll(tile(grecv.at[0, ey, c], 0), 64, 1))
                for ex, ghost in ((0, down), (1, up)):
                    y = tile(tot.at[c, ex, ey], t) + ghost
                    above = pltpu.roll(pltpu.roll(y, 7, 1), 15, 0)
                    below = pltpu.roll(pltpu.roll(y, 121, 1), 1, 0)
                    y = y + jnp.where(z_up, above, jnp.where(z_down, below, 0.0))
                    ztot[c, ex, ey, t * 8:t * 8 + 8, :] = y[:8]
                    ztot[c, ex, ey, 32 + t * 8:40 + t * 8, :] = y[8:]
        return 0

    lax.fori_loop(0, 2, add_ghost, 0)

    lane8 = lax.broadcasted_iota(I32, (8, 128), 1)
    j8 = lax.rem(lane8 // 8, 8)
    for c in range(3):
        for h in range(2):
            lo_face = jnp.zeros((8, 128), F32)
            hi_face = jnp.zeros((8, 128), F32)
            for ex in range(2):
                for t in range(4):
                    n = ex * 4 + t
                    rows = slice(h * 32 + t * 8, h * 32 + t * 8 + 8)
                    lo_face = jnp.where(j8 == n, rolled(ztot[c, ex, 0, rows, :], 8 * n, 1), lo_face)
                    hi_face = jnp.where(j8 == n, rolled(ztot[c, ex, 3, rows, :], 8 * n - 56, 1), hi_face)
            ysend[0, (c * 2 + h) * 8:(c * 2 + h) * 8 + 8, :] = lo_face
            ysend[1, (c * 2 + h) * 8:(c * 2 + h) * 8 + 8, :] = hi_face

    def y_copy(way):
        return pltpu.make_async_remote_copy(
            src_ref=ysend.at[way], dst_ref=yrecv.at[way], send_sem=y_ss.at[way], recv_sem=y_rs.at[way],
            device_id={"gy": me - 1 if way == 0 else me + 1}, device_id_type=MESH)

    @pl.when(has_lo)
    def _():
        y_copy(0).start()

    @pl.when(has_hi)
    def _():
        y_copy(1).start()

    lax.fori_loop(2, 4, add_ghost, 0)

    @pl.when(has_hi)
    def _():
        y_copy(0).wait_recv()

    @pl.when(jnp.logical_not(has_hi))
    def _():
        yrecv[0] = jnp.zeros((48, 128), F32)

    @pl.when(has_lo)
    def _():
        y_copy(1).wait_recv()

    @pl.when(jnp.logical_not(has_lo))
    def _():
        yrecv[1] = jnp.zeros((48, 128), F32)

    def finish(c, _):
        for ex in range(2):
            for t in range(4):
                n = ex * 4 + t
                lo_rows = slice(t * 8, t * 8 + 8)
                hi_rows = slice(32 + t * 8, 32 + t * 8 + 8)
                x = [jnp.concatenate([ztot[c, ex, ey, lo_rows, :], ztot[c, ex, ey, hi_rows, :]], axis=0)
                     for ey in range(4)]
                face = pl.ds(pl.multiple_of(c * 16, 16), 16)
                from_hi = rolled(yrecv[0, face, :], 56 - 8 * n, 1)
                from_lo = rolled(yrecv[1, face, :], -8 * n, 1)
                for ey in range(4):
                    nxt = from_hi if ey == 3 else pltpu.roll(x[ey + 1], 56, 1)
                    prv = from_lo if ey == 0 else pltpu.roll(x[ey - 1], 72, 1)
                    src_out[c, ex, ey, :, t * 128:(t + 1) * 128] = x[ey] + jnp.where(
                        j16 == 7, nxt, jnp.where(j16 == 0, prv, 0.0))
        return 0

    lax.fori_loop(0, 3, finish, 0)

    for k in (1, 2, 3):
        dat_copy(k).wait_send()

    for ey in range(4):
        @pl.when(has_prev)
        def _():
            gm_copy(ey).wait_send()

        @pl.when(has_next)
        def _():
            gp_copy(ey).wait_send()

    @pl.when(has_lo)
    def _():
        y_copy(0).wait_send()

    @pl.when(has_hi)
    def _():
        y_copy(1).wait_send()


def body(velocity, part_pos, part_vel, part_coef, counts, dest, elem):
    vm = pl.BlockSpec(memory_space=pltpu.VMEM)
    hbm = pl.BlockSpec(memory_space=pltpu.HBM)
    dma = pltpu.SemaphoreType.DMA
    drag, source = pl.pallas_call(
        kernel,
        out_shape=(
            jax.ShapeDtypeStruct((3, 128, 128), F32),
            jax.ShapeDtypeStruct(velocity.shape, F32),
        ),
        in_specs=[hbm] * 7,
        out_specs=(vm, vm),
        scratch_shapes=[
            pltpu.VMEM((3, 2, 4, 16, 512), BF16),
            pltpu.VMEM((3, 128, 128), F32),
            pltpu.VMEM((3, 128, 128), F32),
            pltpu.VMEM((128, 2, 128), F32),
            pltpu.SMEM((128,), I32),
            pltpu.VMEM((1, 128), I32),
            pltpu.VMEM((1, 128), I32),
            dma((7,)),
            pltpu.VMEM((4, 256, 128), F32),
            pltpu.VMEM((4, 256, 128), F32),
            pltpu.VMEM((4, 1, 128), I32),
            pltpu.VMEM((4, 1, 128), I32),
            pltpu.VMEM((8, 128), I32),
            pltpu.SMEM((8, 128), I32),
            pltpu.VMEM((128, 128), I32),
            pltpu.VMEM((3072, 128), F32),
            pltpu.VMEM((3, 1024, 128), F32),
            pltpu.VMEM((6, 1024, 128), F32),
            pltpu.VMEM((3, 128, 128), F32),
            pltpu.VMEM((384, 128), F32),
            pltpu.VMEM((384, 128), F32),
            pltpu.VMEM((3, 2, 4, 64, 128), F32),
            pltpu.VMEM((3, 2, 4, 64, 128), F32),
            pltpu.VMEM((2, 4, 3, 64, 128), F32),
            pltpu.VMEM((2, 4, 3, 64, 128), F32),
            pltpu.VMEM((2, 48, 128), F32),
            pltpu.VMEM((2, 48, 128), F32),
            dma((1,)), dma((4,)), dma((4,)), dma((4,)), dma((4,)), dma((4,)), dma((4,)),
            dma((4,)), dma((4,)), dma((4,)), dma((4,)), dma((2,)), dma((2,)),
        ],
        compiler_params=pltpu.CompilerParams(
            collective_id=0, has_side_effects=True, vmem_limit_bytes=67043328),
    )(velocity, part_pos.transpose(1, 0, 2), part_vel.transpose(1, 0, 2), part_coef, counts,
      dest.reshape(1, 128), elem.reshape(1, 128))
    return drag.transpose(1, 0, 2), source


def solution(mesh):
    in_specs = (
        P(None, "gx", "gy", None, None),
        P(("gx", "gy"), None, None),
        P(("gx", "gy"), None, None),
        P(("gx", "gy"), None, None),
        P(("gx", "gy")),
        P(("gx", "gy")),
        P(("gx", "gy")),
    )
    out_specs = (P(("gx", "gy"), None, None), P(None, "gx", "gy", None, None))
    return jax.shard_map(body, mesh=mesh, in_specs=in_specs, out_specs=out_specs, check_vma=False)
```

```python
import functools

import jax
import jax.numpy as jnp
from jax import lax
from jax.experimental import pallas as pl
from jax.experimental.pallas import tpu as pltpu
from jax.sharding import PartitionSpec as P

GLL = (
    -1.0,
    -0.8717401485096066,
    -0.5917001814331423,
    -0.2092992179024789,
    0.2092992179024789,
    0.5917001814331423,
    0.8717401485096066,
    1.0,
)
SHARPNESS = 8.0
MESH = pl.DeviceIdType.MESH
F32 = jnp.float32
BF16 = jnp.bfloat16
I32 = jnp.int32
ROW = tuple((i % 2) * 4 + i // 2 for i in range(8))


def norm_consts():
    out = []
    for i in range(8):
        p = 1.0
        for m in range(8):
            if m != i:
                p *= GLL[i] - GLL[m]
        out.append(1.0 / p)
    return out


NORM = norm_consts()


def lagrange_all(x):
    d = [x - q for q in GLL]
    pre = [None] * 8
    suf = [None] * 8
    for i in range(1, 8):
        pre[i] = d[i - 1] if i == 1 else pre[i - 1] * d[i - 1]
    for i in range(6, -1, -1):
        suf[i] = d[i + 1] if i == 6 else suf[i + 1] * d[i + 1]
    out = []
    for i in range(8):
        if i == 0:
            v = suf[0]
        elif i == 7:
            v = pre[7]
        else:
            v = pre[i] * suf[i]
        out.append(v * NORM[i])
    return out


def gauss_all(x):
    return [jnp.exp(-SHARPNESS * (q - x) * (q - x)) for q in GLL]


def split_bf16(x):
    hi = x.astype(BF16)
    lo = (x - hi.astype(F32)).astype(BF16)
    return hi, lo


def rolled(x, by, axis):
    size = x.shape[axis]
    by = by % size
    if by == 0:
        return x
    return pltpu.roll(x, by, axis)


def kernel(
    field_h, pos_h, vel_h, coef_h, counts_h, dest_h, elem_h,
    drag_h, ztot_h, face_h,
    field, pos, vel, coef, counts, dest, elem, in_sem, drag_out, out_sem,
    send, recv, lab_send, lab_recv, perm_v, perm_s, gt_v, fbuf, lag, gau, fluid, drag_s, ret,
    tot, ztot, gsend, grecv, ysend, yrecv,
    sm_sem, lab_ss, lab_rs, pos_ss, pos_rs, dat_ss, dat_rs, ret_ss, ret_rs, gm_ss, gm_rs, gp_ss, gp_rs, y_ss, y_rs,
):
    gx = lax.axis_index("gx")
    me = lax.axis_index("gy")
    n_gx = lax.axis_size("gx")
    n_gy = lax.axis_size("gy")
    has_prev = gx > 0
    has_next = gx < n_gx - 1
    has_lo = me > 0
    has_hi = me < n_gy - 1

    ins = [
        pltpu.make_async_copy(a, b, in_sem.at[n])
        for n, (a, b) in enumerate((
            (dest_h, dest), (elem_h, elem), (counts_h, counts), (pos_h, pos), (vel_h, vel), (coef_h, coef),
            (field_h, field)))
    ]
    for copy in ins:
        copy.start()

    bar = pltpu.get_barrier_semaphore()
    for k in (1, 2, 3):
        pl.semaphore_signal(bar, inc=1, device_id={"gy": lax.rem(me + k, 4)}, device_id_type=MESH)

    @pl.when(has_prev)
    def _():
        pl.semaphore_signal(bar, inc=1, device_id={"gx": gx - 1}, device_id_type=MESH)

    @pl.when(has_next)
    def _():
        pl.semaphore_signal(bar, inc=1, device_id={"gx": gx + 1}, device_id_type=MESH)

    sub = lax.broadcasted_iota(I32, (128, 128), 0)
    lane = lax.broadcasted_iota(I32, (128, 128), 1)
    ins[0].wait()
    ins[1].wait()
    d_row = dest[...]
    d_b = jnp.broadcast_to(d_row, (128, 128))
    d_t = d_b.T
    before = jnp.where((d_b == d_t) & (sub < lane), 1, 0)
    rank = jnp.sum(before, axis=0, keepdims=True)
    place = d_row * 32 + rank
    p_t = jnp.broadcast_to(place, (128, 128)).T
    e_t = jnp.broadcast_to(elem[...], (128, 128)).T
    perm_v[0:1, :] = jnp.max(jnp.where(p_t == lane, sub, 0), axis=0, keepdims=True)
    perm_v[1:2, :] = d_row * 96 + rank
    to_smem = pltpu.make_async_copy(perm_v, perm_s, sm_sem.at[0])
    to_smem.start()
    mine = (lane >= me * 32) & (lane < me * 32 + 32)
    for k in range(4):
        d = lax.rem(me + k, 4)
        target = lane + (d - me) * 32
        row = jnp.max(jnp.where((p_t == target) & mine, e_t, 0), axis=0, keepdims=True)
        if k == 0:
            lab_recv[me] = row
        else:
            lab_send[k] = row

    def lab_copy(k):
        return pltpu.make_async_remote_copy(
            src_ref=lab_send.at[k], dst_ref=lab_recv.at[me],
            send_sem=lab_ss.at[k], recv_sem=lab_rs.at[lax.rem(4 - k, 4)],
            device_id={"gy": lax.rem(me + k, 4)}, device_id_type=MESH)

    def pos_copy(k):
        return pltpu.make_async_remote_copy(
            src_ref=send.at[k, pl.ds(0, 96)], dst_ref=recv.at[me, pl.ds(0, 96)],
            send_sem=pos_ss.at[k], recv_sem=pos_rs.at[lax.rem(4 - k, 4)],
            device_id={"gy": lax.rem(me + k, 4)}, device_id_type=MESH)

    def dat_copy(k):
        return pltpu.make_async_remote_copy(
            src_ref=send.at[k, pl.ds(96, 160)], dst_ref=recv.at[me, pl.ds(96, 160)],
            send_sem=dat_ss.at[k], recv_sem=dat_rs.at[lax.rem(4 - k, 4)],
            device_id={"gy": lax.rem(me + k, 4)}, device_id_type=MESH)

    def ret_copy(k):
        s = lax.rem(me + k, 4)
        return pltpu.make_async_remote_copy(
            src_ref=drag_s.at[pl.ds(pl.multiple_of(s * 96, 96), 96)],
            dst_ref=ret.at[pl.ds(pl.multiple_of(me * 96, 96), 96)],
            send_sem=ret_ss.at[k], recv_sem=ret_rs.at[lax.rem(4 - k, 4)],
            device_id={"gy": s}, device_id_type=MESH)

    slot_lane = lax.broadcasted_iota(I32, (1, 128), 1)

    def pack_pos(dst, at, d):
        def step(g, _):
            for u in range(8):
                m = g * 8 + u
                b = perm_s[0, d * 32 + m]
                for c in range(3):
                    dst[at, pl.ds(c * 32 + m, 1), :] = pos[c, pl.ds(b, 1), :]
            return 0

        lax.fori_loop(0, 4, step, 0)

    def pack_rest(dst, at, d):
        def step(g, _):
            for u in range(8):
                m = g * 8 + u
                b = perm_s[0, d * 32 + m]
                live = slot_lane < counts[b]
                c2 = coef[b]
                for c in range(3):
                    dst[at, pl.ds(96 + c * 32 + m, 1), :] = vel[c, pl.ds(b, 1), :]
                dst[at, pl.ds(192 + m, 1), :] = jnp.where(live, c2[0:1], 0.0)
                dst[at, pl.ds(224 + m, 1), :] = c2[1:2]
            return 0

        lax.fori_loop(0, 4, step, 0)

    def third(q):
        return 2 - q + 3 * (q // 2)

    to_smem.wait()
    ins[3].wait()

    def pack_pos_to(q, _):
        k = third(q)
        pack_pos(send, k, lax.rem(me + k, 4))
        return 0

    lax.fori_loop(0, 3, pack_pos_to, 0)
    pl.semaphore_wait(bar, 3 + (gx + n_gx - 1) // n_gx + (2 * n_gx - 2 - gx) // n_gx)

    for k in (2, 1, 3):
        lab_copy(k).start()
    for k in (2, 1, 3):
        pos_copy(k).start()
    for n in (2, 4, 5):
        ins[n].wait()

    def pack_and_send(q, _):
        k = third(q)
        pack_rest(send, k, lax.rem(me + k, 4))
        dat_copy(k).start()
        return 0

    lax.fori_loop(0, 3, pack_and_send, 0)
    pack_pos(recv, me, me)
    pack_rest(recv, me, me)

    half = lax.broadcasted_iota(I32, (16, 128), 1) < 64

    ins[6].wait()

    def spread_field(n, _):
        c = n // 8
        ex = lax.rem(n // 4, 2)
        ey = lax.rem(n, 4)
        base = (ex * 4 + ey) * 16 * 24 + c * 8
        for t in range(4):
            x = field[c, ex, ey, :, t * 128:(t + 1) * 128].astype(F32)
            y = pltpu.roll(x, 64, 1)
            fbuf[pl.ds(base + t, 16, stride=24), :] = jnp.where(half, x, y)
            fbuf[pl.ds(base + 4 + t, 16, stride=24), :] = jnp.where(half, y, x)
        return 0

    lax.fori_loop(0, 24, spread_field, 0)

    for k in (1, 3, 2):
        lab_copy(k).wait()
    labels = lab_recv[0] + lab_recv[1] + lab_recv[2] + lab_recv[3]
    g_t = jnp.broadcast_to(labels, (128, 128)).T
    gt_v[...] = g_t
    inv = jnp.max(jnp.where(g_t == lane, sub, 0), axis=0, keepdims=True)
    perm_v[2:3, :] = labels
    perm_v[3:4, :] = inv
    perm_v[4:5, :] = (inv // 32) * 96 + lax.rem(inv, 32)
    to_smem = pltpu.make_async_copy(perm_v, perm_s, sm_sem.at[0])
    to_smem.start()
    to_smem.wait()

    hp = jnp.where(has_prev, 1.0, 0.0).astype(F32)
    hn = jnp.where(has_next, 1.0, 0.0).astype(F32)

    def chunk(q, _):
        k = lax.rem((q * q + q) // 2, 4)
        s = lax.rem(me + k, 4)

        @pl.when(q > 0)
        def _():
            pos_copy(lax.rem(4 - k, 4)).wait_recv()

        def bulk(g, _):
            first = s * 32 + g * 8

            def rows_of(r):
                return recv[s, pl.ds(pl.multiple_of(r * 32 + g * 8, 8), 8), :]

            def put(ref, kind, row, v):
                ref[kind, pl.ds(first * 8 + row, 8, stride=8), :] = v

            r, sc, tc = rows_of(0), rows_of(1), rows_of(2)
            lr, ls, lt = lagrange_all(r), lagrange_all(sc), lagrange_all(tc)
            for i in range(8):
                put(lag, 0, ROW[i], lr[i])
                put(lag, 1, i, ls[i])
                put(lag, 2, i, lt[i])
            ex0 = gt_v[pl.ds(pl.multiple_of(first, 8), 8), :] < 64
            own, minus, plus = gauss_all(r), gauss_all(r + 2.0), gauss_all(r - 2.0)
            zero = jnp.zeros_like(r)
            for i in range(8):
                o, p, m, x = own[i], plus[i], minus[i], zero
                if i == 0:
                    o = o + jnp.where(ex0, hp * minus[7], minus[7])
                    p = p + own[7]
                    x = jnp.where(ex0, plus[7], 0.0)
                if i == 7:
                    o = o + jnp.where(ex0, plus[0], hn * plus[0])
                    m = m + own[0]
                    x = jnp.where(ex0, 0.0, minus[0])
                put(gau, 0, ROW[i], o)
                put(gau, 1, ROW[i], p)
                put(gau, 2, ROW[i], m)
                put(gau, 3, ROW[i], x)
            gs, gt = gauss_all(sc), gauss_all(tc)
            for i in range(8):
                put(gau, 4, i, gs[i])
                put(gau, 5, i, gt[i])
            return 0

        lax.fori_loop(0, 4, bulk, 0)

        def interp(g, _):
            for u in range(32):
                slot = s * 32 + g * 32 + u
                e = perm_s[2, slot]
                f = fbuf[pl.ds(e * 24, 24), :].astype(BF16)
                at = pl.multiple_of(slot * 8, 8)
                lt = lag[2, pl.ds(at, 8), :]
                ls = lag[1, pl.ds(at, 8), :]
                plane = jnp.concatenate([ls[j:j + 1] * lt for j in range(8)], axis=0)
                hi, lo = split_bf16(plane)
                out = jnp.dot(f, jnp.concatenate([hi, lo], axis=0), preferred_element_type=F32)
                lr = lag[0, pl.ds(at, 8), :]
                for c in range(3):
                    fluid[c, pl.ds(slot, 1), :] = jnp.sum(out[8 * c:8 * c + 8] * lr, axis=0, keepdims=True)
            return 0

        interp(0, 0)
        return 0

    lax.fori_loop(0, 4, chunk, 0)

    def drags(q, _):
        k = lax.rem((q * q + q) // 2, 4)
        s = lax.rem(me + k, 4)

        @pl.when(q > 0)
        def _():
            dat_copy(lax.rem(4 - k, 4)).wait_recv()

        rel = []
        for c in range(3):
            rel.append(fluid[c, pl.ds(pl.multiple_of(s * 32, 32), 32), :]
                       - recv[s, 96 + c * 32:128 + c * 32, :])
        speed = jnp.sqrt(rel[0] * rel[0] + rel[1] * rel[1] + rel[2] * rel[2])
        reynolds = jnp.maximum(recv[s, 224:256, :] * speed, 1e-30)
        factor = recv[s, 192:224, :] * (1.0 + 0.15 * jnp.exp(0.687 * jnp.log(reynolds)))
        for c in range(3):
            drag_s[pl.ds(pl.multiple_of(s * 96 + c * 32, 32), 32), :] = factor * rel[c]

        @pl.when(q > 0)
        def _():
            ret_copy(k).start()
        return 0

    lax.fori_loop(0, 4, drags, 0)
    own_rows = pl.ds(pl.multiple_of(me * 96, 96), 96)
    ret[own_rows, :] = drag_s[own_rows, :]

    half8 = lax.broadcasted_iota(I32, (8, 128), 1) < 64

    def gm_copy(ey):
        return pltpu.make_async_remote_copy(
            src_ref=gsend.at[0, ey], dst_ref=grecv.at[0, ey], send_sem=gm_ss.at[ey], recv_sem=gm_rs.at[ey],
            device_id={"gx": gx - 1}, device_id_type=MESH)

    def gp_copy(ey):
        return pltpu.make_async_remote_copy(
            src_ref=gsend.at[1, ey], dst_ref=grecv.at[1, ey], send_sem=gp_ss.at[ey], recv_sem=gp_rs.at[ey],
            device_id={"gx": gx + 1}, device_id_type=MESH)

    def weights(slot, drow, order):
        at = slot * 8
        gs = gau[4, pl.ds(at, 8), :]
        gt = gau[5, pl.ds(at, 8), :]
        plane = jnp.concatenate([gs[j:j + 1] * gt for j in range(8)], axis=0)
        hi, lo = split_bf16(plane)
        rhs = jnp.concatenate([hi, lo], axis=0)
        d = [jnp.broadcast_to(-drag_s[pl.ds(drow + c * 32, 1), :], (8, 128)) for c in range(3)]
        w = [gau[n, pl.ds(at, 8), :] for n in order]
        lhs = jnp.concatenate([a * d[c] for a in w for c in range(3)], axis=0)
        lhi, llo = split_bf16(lhs)
        return rhs, lhi, llo

    def deposit_row(q, _):
        ey = lax.rem(3 * q, 4)

        def pair_group(g, _):
            for u in range(16):
                ez = g * 16 + u
                e0 = ey * 16 + ez
                e1 = 64 + e0
                r0, h0, l0 = weights(perm_s[3, e0], perm_s[4, e0], (0, 1, 2, 3))
                r1, h1, l1 = weights(perm_s[3, e1], perm_s[4, e1], (2, 0, 3, 1))
                lhs = jnp.concatenate(
                    [jnp.concatenate([h0, h1], axis=1), jnp.concatenate([l0, l1], axis=1)], axis=0)
                rhs = jnp.concatenate([r0, r1], axis=1)
                out = lax.dot_general(lhs, rhs, (((1,), (1,)), ((), ())), preferred_element_type=F32)
                z = out[0:96] + out[96:192]
                z = z + pltpu.roll(z, 64, 1)
                ezh, ezl = ez // 8, ez % 8
                for o in range(4):
                    for c in range(3):
                        v = z[(o * 3 + c) * 8:(o * 3 + c) * 8 + 8]
                        v = jnp.where(half8, v, pltpu.roll(v, 4, 0))[0:4]
                        if o < 2:
                            tot[c, o, ey, pl.ds(ezh * 32 + ezl, 4, stride=8), :] = v
                        else:
                            gsend[o - 2, ey, c, pl.ds(ezh * 32 + ezl, 4, stride=8), :] = v
            return 0

        pair_group(0, 0)

        @pl.when(has_prev)
        def _():
            gm_copy(ey).start()

        @pl.when(has_next)
        def _():
            gp_copy(ey).start()
        return 0

    lax.fori_loop(0, 4, deposit_row, 0)

    for k in (1, 3, 2):
        ret_copy(k).wait()

    def unpack(g, _):
        for u in range(8):
            b = g * 8 + u
            row = perm_s[1, b]
            for c in range(3):
                drag_out[c, pl.ds(b, 1), :] = ret[pl.ds(row + c * 32, 1), :]
        return 0

    lax.fori_loop(0, 16, unpack, 0)

    drag_done = pltpu.make_async_copy(drag_out, drag_h, out_sem.at[6])
    drag_done.start()

    def z_copy(ey):
        return pltpu.make_async_copy(ztot.at[:, :, ey], ztot_h.at[:, :, ey], out_sem.at[ey])

    lane16 = lax.broadcasted_iota(I32, (16, 128), 1)
    row16 = lax.broadcasted_iota(I32, (16, 128), 0)
    j16 = lax.rem(lane16 // 8, 8)
    half16 = lane16 < 64
    k16 = lax.rem(lane16, 8)
    z_up = (k16 == 7) & (row16 < 15)
    z_down = (k16 == 0) & (row16 > 0)

    def add_ghost(q, _):
        ey = lax.rem(3 * q, 4)

        @pl.when(has_next)
        def _():
            gm_copy(ey).wait_recv()

        @pl.when(jnp.logical_not(has_next))
        def _():
            grecv[0, ey] = jnp.zeros((3, 64, 128), F32)

        @pl.when(has_prev)
        def _():
            gp_copy(ey).wait_recv()

        @pl.when(jnp.logical_not(has_prev))
        def _():
            grecv[1, ey] = jnp.zeros((3, 64, 128), F32)

        def tile(ref, t):
            return jnp.concatenate([ref[t * 8:t * 8 + 8, :], ref[32 + t * 8:40 + t * 8, :]], axis=0)

        for c in range(3):
            for t in range(4):
                up = tile(grecv.at[0, ey, c], t)
                down = tile(grecv.at[1, ey, c], t)
                if t == 0:
                    up = up + jnp.where(half16, pltpu.roll(tile(grecv.at[1, ey, c], 3), 64, 1), 0.0)
                if t == 3:
                    down = down + jnp.where(half16, 0.0, pltpu.roll(tile(grecv.at[0, ey, c], 0), 64, 1))
                for ex, ghost in ((0, down), (1, up)):
                    y = tile(tot.at[c, ex, ey], t) + ghost
                    above = pltpu.roll(pltpu.roll(y, 7, 1), 15, 0)
                    below = pltpu.roll(pltpu.roll(y, 121, 1), 1, 0)
                    y = y + jnp.where(z_up, above, jnp.where(z_down, below, 0.0))
                    ztot[c, ex, ey, t * 8:t * 8 + 8, :] = y[:8]
                    ztot[c, ex, ey, 32 + t * 8:40 + t * 8, :] = y[8:]
        z_copy(ey).start()
        return 0

    lax.fori_loop(0, 2, add_ghost, 0)

    lane8 = lax.broadcasted_iota(I32, (8, 128), 1)
    j8 = lax.rem(lane8 // 8, 8)
    for c in range(3):
        for h in range(2):
            lo_face = jnp.zeros((8, 128), F32)
            hi_face = jnp.zeros((8, 128), F32)
            for ex in range(2):
                for t in range(4):
                    n = ex * 4 + t
                    rows = slice(h * 32 + t * 8, h * 32 + t * 8 + 8)
                    lo_face = jnp.where(j8 == n, rolled(ztot[c, ex, 0, rows, :], 8 * n, 1), lo_face)
                    hi_face = jnp.where(j8 == n, rolled(ztot[c, ex, 3, rows, :], 8 * n - 56, 1), hi_face)
            ysend[0, (c * 2 + h) * 8:(c * 2 + h) * 8 + 8, :] = lo_face
            ysend[1, (c * 2 + h) * 8:(c * 2 + h) * 8 + 8, :] = hi_face

    def y_copy(way):
        return pltpu.make_async_remote_copy(
            src_ref=ysend.at[way], dst_ref=yrecv.at[way], send_sem=y_ss.at[way], recv_sem=y_rs.at[way],
            device_id={"gy": me - 1 if way == 0 else me + 1}, device_id_type=MESH)

    @pl.when(has_lo)
    def _():
        y_copy(0).start()

    @pl.when(has_hi)
    def _():
        y_copy(1).start()

    lax.fori_loop(2, 4, add_ghost, 0)

    @pl.when(has_hi)
    def _():
        y_copy(0).wait_recv()

    @pl.when(jnp.logical_not(has_hi))
    def _():
        yrecv[0] = jnp.zeros((48, 128), F32)

    @pl.when(has_lo)
    def _():
        y_copy(1).wait_recv()

    @pl.when(jnp.logical_not(has_lo))
    def _():
        yrecv[1] = jnp.zeros((48, 128), F32)

    faces = [pltpu.make_async_copy(yrecv.at[way], face_h.at[way], out_sem.at[4 + way]) for way in range(2)]
    for copy in faces:
        copy.start()

    for k in (1, 2, 3):
        pos_copy(k).wait_send()
        dat_copy(k).wait_send()

    for ey in range(4):
        @pl.when(has_prev)
        def _():
            gm_copy(ey).wait_send()

        @pl.when(has_next)
        def _():
            gp_copy(ey).wait_send()

    @pl.when(has_lo)
    def _():
        y_copy(0).wait_send()

    @pl.when(has_hi)
    def _():
        y_copy(1).wait_send()
    drag_done.wait()
    for ey in range(4):
        z_copy(ey).wait()
    for copy in faces:
        copy.wait()


def finish(drag_in, ztot, yrecv, drag_out, src_out):
    drag_out[...] = drag_in[...]
    lane16 = lax.broadcasted_iota(I32, (16, 128), 1)
    j16 = lax.rem(lane16 // 8, 8)
    for ex in range(2):
        for t in range(4):
            n = ex * 4 + t
            lo_rows = slice(t * 8, t * 8 + 8)
            hi_rows = slice(32 + t * 8, 32 + t * 8 + 8)
            x = [jnp.concatenate([ztot[0, ex, ey, lo_rows, :], ztot[0, ex, ey, hi_rows, :]], axis=0)
                 for ey in range(4)]
            from_hi = rolled(yrecv[0], 56 - 8 * n, 1)
            from_lo = rolled(yrecv[1], -8 * n, 1)
            for ey in range(4):
                nxt = from_hi if ey == 3 else pltpu.roll(x[ey + 1], 56, 1)
                prv = from_lo if ey == 0 else pltpu.roll(x[ey - 1], 72, 1)
                src_out[0, ex, ey, :, t * 128:(t + 1) * 128] = x[ey] + jnp.where(
                    j16 == 7, nxt, jnp.where(j16 == 0, prv, 0.0))


def body(velocity, part_pos, part_vel, part_coef, counts, dest, elem):
    hbm = pl.BlockSpec(memory_space=pltpu.HBM)
    dma = pltpu.SemaphoreType.DMA
    drag, ztot, face = pl.pallas_call(
        kernel,
        out_shape=(
            jax.ShapeDtypeStruct((3, 128, 128), F32),
            jax.ShapeDtypeStruct((3, 2, 4, 64, 128), F32),
            jax.ShapeDtypeStruct((2, 48, 128), F32),
        ),
        in_specs=[hbm] * 7,
        out_specs=(hbm, hbm, hbm),
        scratch_shapes=[
            pltpu.VMEM((3, 2, 4, 16, 512), BF16),
            pltpu.VMEM((3, 128, 128), F32),
            pltpu.VMEM((3, 128, 128), F32),
            pltpu.VMEM((128, 2, 128), F32),
            pltpu.SMEM((128,), I32),
            pltpu.VMEM((1, 128), I32),
            pltpu.VMEM((1, 128), I32),
            dma((7,)),
            pltpu.VMEM((3, 128, 128), F32),
            dma((7,)),
            pltpu.VMEM((4, 256, 128), F32),
            pltpu.VMEM((4, 256, 128), F32),
            pltpu.VMEM((4, 1, 128), I32),
            pltpu.VMEM((4, 1, 128), I32),
            pltpu.VMEM((8, 128), I32),
            pltpu.SMEM((8, 128), I32),
            pltpu.VMEM((128, 128), I32),
            pltpu.VMEM((3072, 128), F32),
            pltpu.VMEM((3, 1024, 128), F32),
            pltpu.VMEM((6, 1024, 128), F32),
            pltpu.VMEM((3, 128, 128), F32),
            pltpu.VMEM((384, 128), F32),
            pltpu.VMEM((384, 128), F32),
            pltpu.VMEM((3, 2, 4, 64, 128), F32),
            pltpu.VMEM((3, 2, 4, 64, 128), F32),
            pltpu.VMEM((2, 4, 3, 64, 128), F32),
            pltpu.VMEM((2, 4, 3, 64, 128), F32),
            pltpu.VMEM((2, 48, 128), F32),
            pltpu.VMEM((2, 48, 128), F32),
            dma((1,)), dma((4,)), dma((4,)), dma((4,)), dma((4,)), dma((4,)), dma((4,)), dma((4,)), dma((4,)),
            dma((4,)), dma((4,)), dma((4,)), dma((4,)), dma((2,)), dma((2,)),
        ],
        compiler_params=pltpu.CompilerParams(
            collective_id=0, has_side_effects=True, vmem_limit_bytes=67043328),
    )(velocity, part_pos.transpose(1, 0, 2), part_vel.transpose(1, 0, 2), part_coef, counts,
      dest.reshape(1, 128), elem.reshape(1, 128))
    drag, source = pl.pallas_call(
        finish,
        grid=(3,),
        in_specs=[
            pl.BlockSpec((1, 128, 128), lambda c: (c, 0, 0)),
            pl.BlockSpec((1, 2, 4, 64, 128), lambda c: (c, 0, 0, 0, 0)),
            pl.BlockSpec((2, 16, 128), lambda c: (0, c, 0)),
        ],
        out_specs=(
            pl.BlockSpec((1, 128, 128), lambda c: (c, 0, 0)),
            pl.BlockSpec((1, 2, 4, 16, 512), lambda c: (c, 0, 0, 0, 0)),
        ),
        out_shape=(
            jax.ShapeDtypeStruct((3, 128, 128), F32),
            jax.ShapeDtypeStruct(velocity.shape, F32),
        ),
        compiler_params=pltpu.CompilerParams(vmem_limit_bytes=67043328),
    )(drag, ztot, face)
    return drag.transpose(1, 0, 2), source


def solution(mesh):
    in_specs = (
        P(None, "gx", "gy", None, None),
        P(("gx", "gy"), None, None),
        P(("gx", "gy"), None, None),
        P(("gx", "gy"), None, None),
        P(("gx", "gy")),
        P(("gx", "gy")),
        P(("gx", "gy")),
    )
    out_specs = (P(("gx", "gy"), None, None), P(None, "gx", "gy", None, None))
    return jax.shard_map(body, mesh=mesh, in_specs=in_specs, out_specs=out_specs, check_vma=False)
```

```python
import functools

import jax
import jax.numpy as jnp
from jax import lax
from jax.experimental import pallas as pl
from jax.experimental.pallas import tpu as pltpu
from jax.sharding import PartitionSpec as P

GLL = (
    -1.0,
    -0.8717401485096066,
    -0.5917001814331423,
    -0.2092992179024789,
    0.2092992179024789,
    0.5917001814331423,
    0.8717401485096066,
    1.0,
)
SHARPNESS = 8.0
MESH = pl.DeviceIdType.MESH
F32 = jnp.float32
BF16 = jnp.bfloat16
I32 = jnp.int32
ROW = tuple((i % 2) * 4 + i // 2 for i in range(8))


def norm_consts():
    out = []
    for i in range(8):
        p = 1.0
        for m in range(8):
            if m != i:
                p *= GLL[i] - GLL[m]
        out.append(1.0 / p)
    return out


NORM = norm_consts()


def lagrange_all(x):
    d = [x - q for q in GLL]
    pre = [None] * 8
    suf = [None] * 8
    for i in range(1, 8):
        pre[i] = d[i - 1] if i == 1 else pre[i - 1] * d[i - 1]
    for i in range(6, -1, -1):
        suf[i] = d[i + 1] if i == 6 else suf[i + 1] * d[i + 1]
    out = []
    for i in range(8):
        if i == 0:
            v = suf[0]
        elif i == 7:
            v = pre[7]
        else:
            v = pre[i] * suf[i]
        out.append(v * NORM[i])
    return out


def gauss_all(x):
    return [jnp.exp(-SHARPNESS * (q - x) * (q - x)) for q in GLL]


def split_bf16(x):
    hi = x.astype(BF16)
    lo = (x - hi.astype(F32)).astype(BF16)
    return hi, lo


def rolled(x, by, axis):
    size = x.shape[axis]
    by = by % size
    if by == 0:
        return x
    return pltpu.roll(x, by, axis)


def kernel(
    field_h, pos_h, vel_h, coef_h, counts_h, dest_h, elem_h,
    drag_h, ztot_h, face_h,
    field, pos, vel, coef, counts, dest, elem, in_sem, drag_out, out_sem,
    send, recv, lab_send, lab_recv, perm_v, perm_s, gt_v, fbuf, lag, gau, fluid, drag_s, ret,
    tot, ztot, gsend, grecv, ysend, yrecv,
    sm_sem, lab_ss, lab_rs, pos_ss, pos_rs, dat_ss, dat_rs, ret_ss, ret_rs, gm_ss, gm_rs, gp_ss, gp_rs, y_ss, y_rs,
):
    gx = lax.axis_index("gx")
    me = lax.axis_index("gy")
    n_gx = lax.axis_size("gx")
    n_gy = lax.axis_size("gy")
    has_prev = gx > 0
    has_next = gx < n_gx - 1
    has_lo = me > 0
    has_hi = me < n_gy - 1

    ins = [
        pltpu.make_async_copy(a, b, in_sem.at[n])
        for n, (a, b) in enumerate((
            (dest_h, dest), (elem_h, elem), (counts_h, counts), (pos_h, pos), (vel_h, vel), (coef_h, coef),
            (field_h, field)))
    ]
    for copy in ins:
        copy.start()

    bar = pltpu.get_barrier_semaphore()
    for k in (1, 2, 3):
        pl.semaphore_signal(bar, inc=1, device_id={"gy": lax.rem(me + k, 4)}, device_id_type=MESH)

    @pl.when(has_prev)
    def _():
        pl.semaphore_signal(bar, inc=1, device_id={"gx": gx - 1}, device_id_type=MESH)

    @pl.when(has_next)
    def _():
        pl.semaphore_signal(bar, inc=1, device_id={"gx": gx + 1}, device_id_type=MESH)

    sub = lax.broadcasted_iota(I32, (128, 128), 0)
    lane = lax.broadcasted_iota(I32, (128, 128), 1)
    ins[0].wait()
    ins[1].wait()
    d_row = dest[...]
    d_b = jnp.broadcast_to(d_row, (128, 128))
    d_t = d_b.T
    before = jnp.where((d_b == d_t) & (sub < lane), 1, 0)
    rank = jnp.sum(before, axis=0, keepdims=True)
    place = d_row * 32 + rank
    p_t = jnp.broadcast_to(place, (128, 128)).T
    e_t = jnp.broadcast_to(elem[...], (128, 128)).T
    perm_v[0:1, :] = jnp.max(jnp.where(p_t == lane, sub, 0), axis=0, keepdims=True)
    perm_v[1:2, :] = d_row * 96 + rank
    to_smem = pltpu.make_async_copy(perm_v, perm_s, sm_sem.at[0])
    to_smem.start()
    mine = (lane >= me * 32) & (lane < me * 32 + 32)
    for k in range(4):
        d = lax.rem(me + k, 4)
        target = lane + (d - me) * 32
        row = jnp.max(jnp.where((p_t == target) & mine, e_t, 0), axis=0, keepdims=True)
        if k == 0:
            lab_recv[me] = row
        else:
            lab_send[k] = row

    def lab_copy(k):
        return pltpu.make_async_remote_copy(
            src_ref=lab_send.at[k], dst_ref=lab_recv.at[me],
            send_sem=lab_ss.at[k], recv_sem=lab_rs.at[lax.rem(4 - k, 4)],
            device_id={"gy": lax.rem(me + k, 4)}, device_id_type=MESH)

    def pos_copy(k):
        return pltpu.make_async_remote_copy(
            src_ref=send.at[k, pl.ds(0, 96)], dst_ref=recv.at[me, pl.ds(0, 96)],
            send_sem=pos_ss.at[k], recv_sem=pos_rs.at[lax.rem(4 - k, 4)],
            device_id={"gy": lax.rem(me + k, 4)}, device_id_type=MESH)

    def dat_copy(k):
        return pltpu.make_async_remote_copy(
            src_ref=send.at[k, pl.ds(96, 160)], dst_ref=recv.at[me, pl.ds(96, 160)],
            send_sem=dat_ss.at[k], recv_sem=dat_rs.at[lax.rem(4 - k, 4)],
            device_id={"gy": lax.rem(me + k, 4)}, device_id_type=MESH)

    def ret_copy(k):
        s = lax.rem(me + k, 4)
        return pltpu.make_async_remote_copy(
            src_ref=drag_s.at[pl.ds(pl.multiple_of(s * 96, 96), 96)],
            dst_ref=ret.at[pl.ds(pl.multiple_of(me * 96, 96), 96)],
            send_sem=ret_ss.at[k], recv_sem=ret_rs.at[lax.rem(4 - k, 4)],
            device_id={"gy": s}, device_id_type=MESH)

    slot_lane = lax.broadcasted_iota(I32, (1, 128), 1)

    def pack_pos(dst, at, d):
        def step(g, _):
            for u in range(8):
                m = g * 8 + u
                b = perm_s[0, d * 32 + m]
                for c in range(3):
                    dst[at, pl.ds(c * 32 + m, 1), :] = pos[c, pl.ds(b, 1), :]
            return 0

        lax.fori_loop(0, 4, step, 0)

    def pack_rest(dst, at, d):
        def step(g, _):
            for u in range(8):
                m = g * 8 + u
                b = perm_s[0, d * 32 + m]
                live = slot_lane < counts[b]
                c2 = coef[b]
                for c in range(3):
                    dst[at, pl.ds(96 + c * 32 + m, 1), :] = vel[c, pl.ds(b, 1), :]
                dst[at, pl.ds(192 + m, 1), :] = jnp.where(live, c2[0:1], 0.0)
                dst[at, pl.ds(224 + m, 1), :] = c2[1:2]
            return 0

        lax.fori_loop(0, 4, step, 0)

    def third(q):
        return 2 - q + 3 * (q // 2)

    to_smem.wait()
    ins[3].wait()

    def pack_pos_to(q, _):
        k = third(q)
        pack_pos(send, k, lax.rem(me + k, 4))
        return 0

    lax.fori_loop(0, 3, pack_pos_to, 0)
    pl.semaphore_wait(bar, 3 + (gx + n_gx - 1) // n_gx + (2 * n_gx - 2 - gx) // n_gx)

    for k in (2, 1, 3):
        lab_copy(k).start()
    for k in (2, 1, 3):
        pos_copy(k).start()
    for n in (2, 4, 5):
        ins[n].wait()

    def pack_and_send(q, _):
        k = third(q)
        pack_rest(send, k, lax.rem(me + k, 4))
        dat_copy(k).start()
        return 0

    lax.fori_loop(0, 3, pack_and_send, 0)
    pack_pos(recv, me, me)
    pack_rest(recv, me, me)

    half = lax.broadcasted_iota(I32, (16, 128), 1) < 64

    ins[6].wait()

    def spread_field(n, _):
        c = n // 8
        ex = lax.rem(n // 4, 2)
        ey = lax.rem(n, 4)
        base = (ex * 4 + ey) * 16 * 24 + c * 8
        for t in range(4):
            x = field[c, ex, ey, :, t * 128:(t + 1) * 128].astype(F32)
            y = pltpu.roll(x, 64, 1)
            fbuf[pl.ds(base + t, 16, stride=24), :] = jnp.where(half, x, y)
            fbuf[pl.ds(base + 4 + t, 16, stride=24), :] = jnp.where(half, y, x)
        return 0

    lax.fori_loop(0, 24, spread_field, 0)

    for k in (1, 3, 2):
        lab_copy(k).wait()
    labels = lab_recv[0] + lab_recv[1] + lab_recv[2] + lab_recv[3]
    g_t = jnp.broadcast_to(labels, (128, 128)).T
    gt_v[...] = g_t
    inv = jnp.max(jnp.where(g_t == lane, sub, 0), axis=0, keepdims=True)
    perm_v[2:3, :] = labels
    perm_v[3:4, :] = inv
    perm_v[4:5, :] = (inv // 32) * 96 + lax.rem(inv, 32)
    to_smem = pltpu.make_async_copy(perm_v, perm_s, sm_sem.at[0])
    to_smem.start()
    to_smem.wait()

    hp = jnp.where(has_prev, 1.0, 0.0).astype(F32)
    hn = jnp.where(has_next, 1.0, 0.0).astype(F32)

    def chunk(q, _):
        k = lax.rem((q * q + q) // 2, 4)
        s = lax.rem(me + k, 4)

        @pl.when(q > 0)
        def _():
            pos_copy(lax.rem(4 - k, 4)).wait_recv()

        def bulk(g, _):
            first = s * 32 + g * 8

            def rows_of(r):
                return recv[s, pl.ds(pl.multiple_of(r * 32 + g * 8, 8), 8), :]

            def put(ref, kind, row, v):
                ref[kind, pl.ds(first * 8 + row, 8, stride=8), :] = v

            r, sc, tc = rows_of(0), rows_of(1), rows_of(2)
            lr, ls, lt = lagrange_all(r), lagrange_all(sc), lagrange_all(tc)
            for i in range(8):
                put(lag, 0, ROW[i], lr[i])
                put(lag, 1, i, ls[i])
                put(lag, 2, i, lt[i])
            ex0 = gt_v[pl.ds(pl.multiple_of(first, 8), 8), :] < 64
            own, minus, plus = gauss_all(r), gauss_all(r + 2.0), gauss_all(r - 2.0)
            zero = jnp.zeros_like(r)
            for i in range(8):
                o, p, m, x = own[i], plus[i], minus[i], zero
                if i == 0:
                    o = o + jnp.where(ex0, hp * minus[7], minus[7])
                    p = p + own[7]
                    x = jnp.where(ex0, plus[7], 0.0)
                if i == 7:
                    o = o + jnp.where(ex0, plus[0], hn * plus[0])
                    m = m + own[0]
                    x = jnp.where(ex0, 0.0, minus[0])
                put(gau, 0, ROW[i], o)
                put(gau, 1, ROW[i], p)
                put(gau, 2, ROW[i], m)
                put(gau, 3, ROW[i], x)
            gs, gt = gauss_all(sc), gauss_all(tc)
            for i in range(8):
                put(gau, 4, i, gs[i])
                put(gau, 5, i, gt[i])
            return 0

        lax.fori_loop(0, 4, bulk, 0)

        def interp(g, _):
            for u in range(32):
                slot = s * 32 + g * 32 + u
                e = perm_s[2, slot]
                f = fbuf[pl.ds(e * 24, 24), :].astype(BF16)
                at = pl.multiple_of(slot * 8, 8)
                lt = lag[2, pl.ds(at, 8), :]
                ls = lag[1, pl.ds(at, 8), :]
                plane = jnp.concatenate([ls[j:j + 1] * lt for j in range(8)], axis=0)
                hi, lo = split_bf16(plane)
                out = jnp.dot(f, jnp.concatenate([hi, lo], axis=0), preferred_element_type=F32)
                lr = lag[0, pl.ds(at, 8), :]
                for c in range(3):
                    fluid[c, pl.ds(slot, 1), :] = jnp.sum(out[8 * c:8 * c + 8] * lr, axis=0, keepdims=True)
            return 0

        interp(0, 0)
        return 0

    lax.fori_loop(0, 4, chunk, 0)

    def drags(q, _):
        k = lax.rem((q * q + q) // 2, 4)
        s = lax.rem(me + k, 4)

        @pl.when(q > 0)
        def _():
            dat_copy(lax.rem(4 - k, 4)).wait_recv()

        rel = []
        for c in range(3):
            rel.append(fluid[c, pl.ds(pl.multiple_of(s * 32, 32), 32), :]
                       - recv[s, 96 + c * 32:128 + c * 32, :])
        speed = jnp.sqrt(rel[0] * rel[0] + rel[1] * rel[1] + rel[2] * rel[2])
        reynolds = jnp.maximum(recv[s, 224:256, :] * speed, 1e-30)
        factor = recv[s, 192:224, :] * (1.0 + 0.15 * jnp.exp(0.687 * jnp.log(reynolds)))
        for c in range(3):
            drag_s[pl.ds(pl.multiple_of(s * 96 + c * 32, 32), 32), :] = factor * rel[c]

        @pl.when(q > 0)
        def _():
            ret_copy(k).start()
        return 0

    lax.fori_loop(0, 4, drags, 0)
    own_rows = pl.ds(pl.multiple_of(me * 96, 96), 96)
    ret[own_rows, :] = drag_s[own_rows, :]

    half8 = lax.broadcasted_iota(I32, (8, 128), 1) < 64

    def gm_copy(ey):
        return pltpu.make_async_remote_copy(
            src_ref=gsend.at[0, ey], dst_ref=grecv.at[0, ey], send_sem=gm_ss.at[ey], recv_sem=gm_rs.at[ey],
            device_id={"gx": gx - 1}, device_id_type=MESH)

    def gp_copy(ey):
        return pltpu.make_async_remote_copy(
            src_ref=gsend.at[1, ey], dst_ref=grecv.at[1, ey], send_sem=gp_ss.at[ey], recv_sem=gp_rs.at[ey],
            device_id={"gx": gx + 1}, device_id_type=MESH)

    def weights(slot, drow, order):
        at = slot * 8
        gs = gau[4, pl.ds(at, 8), :]
        gt = gau[5, pl.ds(at, 8), :]
        plane = jnp.concatenate([gs[j:j + 1] * gt for j in range(8)], axis=0)
        hi, lo = split_bf16(plane)
        rhs = jnp.concatenate([hi, lo], axis=0)
        d = [jnp.broadcast_to(-drag_s[pl.ds(drow + c * 32, 1), :], (8, 128)) for c in range(3)]
        w = [gau[n, pl.ds(at, 8), :] for n in order]
        lhs = jnp.concatenate([a * d[c] for a in w for c in range(3)], axis=0)
        lhi, llo = split_bf16(lhs)
        return rhs, lhi, llo

    def deposit_row(q, _):
        ey = lax.rem(3 * q, 4)

        def pair_group(g, _):
            for u in range(16):
                ez = g * 16 + u
                e0 = ey * 16 + ez
                e1 = 64 + e0
                r0, h0, l0 = weights(perm_s[3, e0], perm_s[4, e0], (0, 1, 2, 3))
                r1, h1, l1 = weights(perm_s[3, e1], perm_s[4, e1], (2, 0, 3, 1))
                lhs = jnp.concatenate(
                    [jnp.concatenate([h0, h1], axis=1), jnp.concatenate([l0, l1], axis=1)], axis=0)
                rhs = jnp.concatenate([r0, r1], axis=1)
                out = lax.dot_general(lhs, rhs, (((1,), (1,)), ((), ())), preferred_element_type=F32)
                z = out[0:96] + out[96:192]
                z = z + pltpu.roll(z, 64, 1)
                ezh, ezl = ez // 8, ez % 8
                for o in range(4):
                    for c in range(3):
                        v = z[(o * 3 + c) * 8:(o * 3 + c) * 8 + 8]
                        v = jnp.where(half8, v, pltpu.roll(v, 4, 0))[0:4]
                        if o < 2:
                            tot[c, o, ey, pl.ds(ezh * 32 + ezl, 4, stride=8), :] = v
                        else:
                            gsend[o - 2, ey, c, pl.ds(ezh * 32 + ezl, 4, stride=8), :] = v
            return 0

        pair_group(0, 0)

        @pl.when(has_prev)
        def _():
            gm_copy(ey).start()

        @pl.when(has_next)
        def _():
            gp_copy(ey).start()
        return 0

    lax.fori_loop(0, 4, deposit_row, 0)

    for k in (1, 3, 2):
        ret_copy(k).wait()

    def unpack(g, _):
        for u in range(8):
            b = g * 8 + u
            row = perm_s[1, b]
            for c in range(3):
                drag_out[c, pl.ds(b, 1), :] = ret[pl.ds(row + c * 32, 1), :]
        return 0

    lax.fori_loop(0, 16, unpack, 0)

    drag_done = pltpu.make_async_copy(drag_out, drag_h, out_sem.at[6])
    drag_done.start()

    def z_copy(ey):
        return pltpu.make_async_copy(ztot.at[:, :, ey], ztot_h.at[:, :, ey], out_sem.at[ey])

    lane16 = lax.broadcasted_iota(I32, (16, 128), 1)
    row16 = lax.broadcasted_iota(I32, (16, 128), 0)
    j16 = lax.rem(lane16 // 8, 8)
    half16 = lane16 < 64
    k16 = lax.rem(lane16, 8)
    z_up = (k16 == 7) & (row16 < 15)
    z_down = (k16 == 0) & (row16 > 0)

    def add_ghost(q, _):
        ey = lax.rem(3 * q, 4)

        @pl.when(has_next)
        def _():
            gm_copy(ey).wait_recv()

        @pl.when(jnp.logical_not(has_next))
        def _():
            grecv[0, ey] = jnp.zeros((3, 64, 128), F32)

        @pl.when(has_prev)
        def _():
            gp_copy(ey).wait_recv()

        @pl.when(jnp.logical_not(has_prev))
        def _():
            grecv[1, ey] = jnp.zeros((3, 64, 128), F32)

        def tile(ref, t):
            return jnp.concatenate([ref[t * 8:t * 8 + 8, :], ref[32 + t * 8:40 + t * 8, :]], axis=0)

        for c in range(3):
            for t in range(4):
                up = tile(grecv.at[0, ey, c], t)
                down = tile(grecv.at[1, ey, c], t)
                if t == 0:
                    up = up + jnp.where(half16, pltpu.roll(tile(grecv.at[1, ey, c], 3), 64, 1), 0.0)
                if t == 3:
                    down = down + jnp.where(half16, 0.0, pltpu.roll(tile(grecv.at[0, ey, c], 0), 64, 1))
                for ex, ghost in ((0, down), (1, up)):
                    y = tile(tot.at[c, ex, ey], t) + ghost
                    above = pltpu.roll(pltpu.roll(y, 7, 1), 15, 0)
                    below = pltpu.roll(pltpu.roll(y, 121, 1), 1, 0)
                    y = y + jnp.where(z_up, above, jnp.where(z_down, below, 0.0))
                    ztot[c, ex, ey, t * 8:t * 8 + 8, :] = y[:8]
                    ztot[c, ex, ey, 32 + t * 8:40 + t * 8, :] = y[8:]
        z_copy(ey).start()
        return 0

    lax.fori_loop(0, 2, add_ghost, 0)

    lane8 = lax.broadcasted_iota(I32, (8, 128), 1)
    j8 = lax.rem(lane8 // 8, 8)
    for c in range(3):
        for h in range(2):
            lo_face = jnp.zeros((8, 128), F32)
            hi_face = jnp.zeros((8, 128), F32)
            for ex in range(2):
                for t in range(4):
                    n = ex * 4 + t
                    rows = slice(h * 32 + t * 8, h * 32 + t * 8 + 8)
                    lo_face = jnp.where(j8 == n, rolled(ztot[c, ex, 0, rows, :], 8 * n, 1), lo_face)
                    hi_face = jnp.where(j8 == n, rolled(ztot[c, ex, 3, rows, :], 8 * n - 56, 1), hi_face)
            ysend[0, (c * 2 + h) * 8:(c * 2 + h) * 8 + 8, :] = lo_face
            ysend[1, (c * 2 + h) * 8:(c * 2 + h) * 8 + 8, :] = hi_face

    def y_copy(way):
        return pltpu.make_async_remote_copy(
            src_ref=ysend.at[way], dst_ref=yrecv.at[way], send_sem=y_ss.at[way], recv_sem=y_rs.at[way],
            device_id={"gy": me - 1 if way == 0 else me + 1}, device_id_type=MESH)

    @pl.when(has_lo)
    def _():
        y_copy(0).start()

    @pl.when(has_hi)
    def _():
        y_copy(1).start()

    lax.fori_loop(2, 4, add_ghost, 0)

    @pl.when(has_hi)
    def _():
        y_copy(0).wait_recv()

    @pl.when(jnp.logical_not(has_hi))
    def _():
        yrecv[0] = jnp.zeros((48, 128), F32)

    @pl.when(has_lo)
    def _():
        y_copy(1).wait_recv()

    @pl.when(jnp.logical_not(has_lo))
    def _():
        yrecv[1] = jnp.zeros((48, 128), F32)

    faces = [pltpu.make_async_copy(yrecv.at[way], face_h.at[way], out_sem.at[4 + way]) for way in range(2)]
    for copy in faces:
        copy.start()

    for k in (1, 2, 3):
        pos_copy(k).wait_send()
        dat_copy(k).wait_send()

    for ey in range(4):
        @pl.when(has_prev)
        def _():
            gm_copy(ey).wait_send()

        @pl.when(has_next)
        def _():
            gp_copy(ey).wait_send()

    @pl.when(has_lo)
    def _():
        y_copy(0).wait_send()

    @pl.when(has_hi)
    def _():
        y_copy(1).wait_send()
    drag_done.wait()
    for ey in range(4):
        z_copy(ey).wait()
    for copy in faces:
        copy.wait()


def finish(drag_h, ztot_h, face_h, drag_o, src_o, drag, ztot, yrecv, src, in_sem, out_sem):
    faces_in = pltpu.make_async_copy(face_h, yrecv, in_sem.at[6])
    drag_in = pltpu.make_async_copy(drag_h, drag, in_sem.at[7])
    drag_done = pltpu.make_async_copy(drag, drag_o, out_sem.at[6])

    def z_in(n):
        return pltpu.make_async_copy(ztot_h.at[n // 2, n % 2], ztot.at[n // 2, n % 2], in_sem.at[n])

    def z_out(n):
        return pltpu.make_async_copy(src.at[n // 2, n % 2], src_o.at[n // 2, n % 2], out_sem.at[n])

    faces_in.start()
    for n in range(6):
        z_in(n).start()
    drag_in.start()
    lane16 = lax.broadcasted_iota(I32, (16, 128), 1)
    j16 = lax.rem(lane16 // 8, 8)
    faces_in.wait()
    for part in range(6):
        c, ex = part // 2, part % 2
        z_in(part).wait()
        for t in range(4):
            n = ex * 4 + t
            lo_rows = slice(t * 8, t * 8 + 8)
            hi_rows = slice(32 + t * 8, 32 + t * 8 + 8)
            x = [jnp.concatenate([ztot[c, ex, ey, lo_rows, :], ztot[c, ex, ey, hi_rows, :]], axis=0)
                 for ey in range(4)]
            from_hi = rolled(yrecv[0, c * 16:c * 16 + 16, :], 56 - 8 * n, 1)
            from_lo = rolled(yrecv[1, c * 16:c * 16 + 16, :], -8 * n, 1)
            for ey in range(4):
                nxt = from_hi if ey == 3 else pltpu.roll(x[ey + 1], 56, 1)
                prv = from_lo if ey == 0 else pltpu.roll(x[ey - 1], 72, 1)
                src[c, ex, ey, :, t * 128:(t + 1) * 128] = x[ey] + jnp.where(
                    j16 == 7, nxt, jnp.where(j16 == 0, prv, 0.0))
        z_out(part).start()
        if part == 1:
            drag_in.wait()
            drag_done.start()
    for n in range(6):
        z_out(n).wait()
    drag_done.wait()


def body(velocity, part_pos, part_vel, part_coef, counts, dest, elem):
    hbm = pl.BlockSpec(memory_space=pltpu.HBM)
    dma = pltpu.SemaphoreType.DMA
    drag, ztot, face = pl.pallas_call(
        kernel,
        out_shape=(
            jax.ShapeDtypeStruct((3, 128, 128), F32),
            jax.ShapeDtypeStruct((3, 2, 4, 64, 128), F32),
            jax.ShapeDtypeStruct((2, 48, 128), F32),
        ),
        in_specs=[hbm] * 7,
        out_specs=(hbm, hbm, hbm),
        scratch_shapes=[
            pltpu.VMEM((3, 2, 4, 16, 512), BF16),
            pltpu.VMEM((3, 128, 128), F32),
            pltpu.VMEM((3, 128, 128), F32),
            pltpu.VMEM((128, 2, 128), F32),
            pltpu.SMEM((128,), I32),
            pltpu.VMEM((1, 128), I32),
            pltpu.VMEM((1, 128), I32),
            dma((7,)),
            pltpu.VMEM((3, 128, 128), F32),
            dma((7,)),
            pltpu.VMEM((4, 256, 128), F32),
            pltpu.VMEM((4, 256, 128), F32),
            pltpu.VMEM((4, 1, 128), I32),
            pltpu.VMEM((4, 1, 128), I32),
            pltpu.VMEM((8, 128), I32),
            pltpu.SMEM((8, 128), I32),
            pltpu.VMEM((128, 128), I32),
            pltpu.VMEM((3072, 128), F32),
            pltpu.VMEM((3, 1024, 128), F32),
            pltpu.VMEM((6, 1024, 128), F32),
            pltpu.VMEM((3, 128, 128), F32),
            pltpu.VMEM((384, 128), F32),
            pltpu.VMEM((384, 128), F32),
            pltpu.VMEM((3, 2, 4, 64, 128), F32),
            pltpu.VMEM((3, 2, 4, 64, 128), F32),
            pltpu.VMEM((2, 4, 3, 64, 128), F32),
            pltpu.VMEM((2, 4, 3, 64, 128), F32),
            pltpu.VMEM((2, 48, 128), F32),
            pltpu.VMEM((2, 48, 128), F32),
            dma((1,)), dma((4,)), dma((4,)), dma((4,)), dma((4,)), dma((4,)), dma((4,)), dma((4,)), dma((4,)),
            dma((4,)), dma((4,)), dma((4,)), dma((4,)), dma((2,)), dma((2,)),
        ],
        compiler_params=pltpu.CompilerParams(
            collective_id=0, has_side_effects=True, vmem_limit_bytes=67043328),
    )(velocity, part_pos.transpose(1, 0, 2), part_vel.transpose(1, 0, 2), part_coef, counts,
      dest.reshape(1, 128), elem.reshape(1, 128))
    drag, source = pl.pallas_call(
        finish,
        in_specs=[hbm] * 3,
        out_specs=(hbm, hbm),
        out_shape=(
            jax.ShapeDtypeStruct((3, 128, 128), F32),
            jax.ShapeDtypeStruct(velocity.shape, F32),
        ),
        scratch_shapes=[
            pltpu.VMEM((3, 128, 128), F32),
            pltpu.VMEM((3, 2, 4, 64, 128), F32),
            pltpu.VMEM((2, 48, 128), F32),
            pltpu.VMEM(velocity.shape, F32),
            dma((8,)), dma((7,)),
        ],
        compiler_params=pltpu.CompilerParams(vmem_limit_bytes=67043328),
    )(drag, ztot, face)
    return drag.transpose(1, 0, 2), source


def solution(mesh):
    in_specs = (
        P(None, "gx", "gy", None, None),
        P(("gx", "gy"), None, None),
        P(("gx", "gy"), None, None),
        P(("gx", "gy"), None, None),
        P(("gx", "gy")),
        P(("gx", "gy")),
        P(("gx", "gy")),
    )
    out_specs = (P(("gx", "gy"), None, None), P(None, "gx", "gy", None, None))
    return jax.shard_map(body, mesh=mesh, in_specs=in_specs, out_specs=out_specs, check_vma=False)
```

```python
import functools

import jax
import jax.numpy as jnp
from jax import lax
from jax.experimental import pallas as pl
from jax.experimental.pallas import tpu as pltpu
from jax.sharding import PartitionSpec as P

GLL = (
    -1.0,
    -0.8717401485096066,
    -0.5917001814331423,
    -0.2092992179024789,
    0.2092992179024789,
    0.5917001814331423,
    0.8717401485096066,
    1.0,
)
SHARPNESS = 8.0
MESH = pl.DeviceIdType.MESH
F32 = jnp.float32
BF16 = jnp.bfloat16
I32 = jnp.int32
ROW = tuple((i % 2) * 4 + i // 2 for i in range(8))


def norm_consts():
    out = []
    for i in range(8):
        p = 1.0
        for m in range(8):
            if m != i:
                p *= GLL[i] - GLL[m]
        out.append(1.0 / p)
    return out


NORM = norm_consts()


def lagrange_all(x):
    d = [x - q for q in GLL]
    pre = [None] * 8
    suf = [None] * 8
    for i in range(1, 8):
        pre[i] = d[i - 1] if i == 1 else pre[i - 1] * d[i - 1]
    for i in range(6, -1, -1):
        suf[i] = d[i + 1] if i == 6 else suf[i + 1] * d[i + 1]
    out = []
    for i in range(8):
        if i == 0:
            v = suf[0]
        elif i == 7:
            v = pre[7]
        else:
            v = pre[i] * suf[i]
        out.append(v * NORM[i])
    return out


def gauss_all(x):
    return [jnp.exp(-SHARPNESS * (q - x) * (q - x)) for q in GLL]


def split_bf16(x):
    hi = x.astype(BF16)
    lo = (x - hi.astype(F32)).astype(BF16)
    return hi, lo


def rolled(x, by, axis):
    size = x.shape[axis]
    by = by % size
    if by == 0:
        return x
    return pltpu.roll(x, by, axis)


def kernel(
    field_h, pos_h, vel_h, coef_h, counts_h, dest_h, elem_h,
    drag_h, ztot_h, face_h,
    field, pos, vel, coef, counts, dest, elem, in_sem, drag_out, out_sem,
    send, recv, lab_send, lab_recv, perm_v, perm_s, gt_v, fbuf, lag, gau, fluid, drag_s, ret,
    tot, ztot, gsend, grecv, ysend, yrecv,
    sm_sem, lab_ss, lab_rs, pos_ss, pos_rs, dat_ss, dat_rs, ret_ss, ret_rs, gm_ss, gm_rs, gp_ss, gp_rs, y_ss, y_rs,
):
    gx = lax.axis_index("gx")
    me = lax.axis_index("gy")
    n_gx = lax.axis_size("gx")
    n_gy = lax.axis_size("gy")
    has_prev = gx > 0
    has_next = gx < n_gx - 1
    has_lo = me > 0
    has_hi = me < n_gy - 1

    ins = [
        pltpu.make_async_copy(a, b, in_sem.at[n])
        for n, (a, b) in enumerate((
            (dest_h, dest), (elem_h, elem), (counts_h, counts), (pos_h, pos), (vel_h, vel), (coef_h, coef),
            (field_h, field)))
    ]
    for copy in ins:
        copy.start()

    bar = pltpu.get_barrier_semaphore()
    for k in (1, 2, 3):
        pl.semaphore_signal(bar, inc=1, device_id={"gy": lax.rem(me + k, 4)}, device_id_type=MESH)

    @pl.when(has_prev)
    def _():
        pl.semaphore_signal(bar, inc=1, device_id={"gx": gx - 1}, device_id_type=MESH)

    @pl.when(has_next)
    def _():
        pl.semaphore_signal(bar, inc=1, device_id={"gx": gx + 1}, device_id_type=MESH)

    sub = lax.broadcasted_iota(I32, (128, 128), 0)
    lane = lax.broadcasted_iota(I32, (128, 128), 1)
    ins[0].wait()
    ins[1].wait()
    d_row = dest[...]
    d_b = jnp.broadcast_to(d_row, (128, 128))
    d_t = d_b.T
    before = jnp.where((d_b == d_t) & (sub < lane), 1, 0)
    rank = jnp.sum(before, axis=0, keepdims=True)
    place = d_row * 32 + rank
    p_t = jnp.broadcast_to(place, (128, 128)).T
    e_t = jnp.broadcast_to(elem[...], (128, 128)).T
    perm_v[0:1, :] = jnp.max(jnp.where(p_t == lane, sub, 0), axis=0, keepdims=True)
    perm_v[1:2, :] = d_row * 96 + rank
    to_smem = pltpu.make_async_copy(perm_v, perm_s, sm_sem.at[0])
    to_smem.start()
    mine = (lane >= me * 32) & (lane < me * 32 + 32)
    for k in range(4):
        d = lax.rem(me + k, 4)
        target = lane + (d - me) * 32
        row = jnp.max(jnp.where((p_t == target) & mine, e_t, 0), axis=0, keepdims=True)
        if k == 0:
            lab_recv[me] = row
        else:
            lab_send[k] = row

    def lab_copy(k):
        return pltpu.make_async_remote_copy(
            src_ref=lab_send.at[k], dst_ref=lab_recv.at[me],
            send_sem=lab_ss.at[k], recv_sem=lab_rs.at[lax.rem(4 - k, 4)],
            device_id={"gy": lax.rem(me + k, 4)}, device_id_type=MESH)

    def pos_copy(k):
        return pltpu.make_async_remote_copy(
            src_ref=send.at[k, pl.ds(0, 96)], dst_ref=recv.at[me, pl.ds(0, 96)],
            send_sem=pos_ss.at[k], recv_sem=pos_rs.at[lax.rem(4 - k, 4)],
            device_id={"gy": lax.rem(me + k, 4)}, device_id_type=MESH)

    def dat_copy(k):
        return pltpu.make_async_remote_copy(
            src_ref=send.at[k, pl.ds(96, 160)], dst_ref=recv.at[me, pl.ds(96, 160)],
            send_sem=dat_ss.at[k], recv_sem=dat_rs.at[lax.rem(4 - k, 4)],
            device_id={"gy": lax.rem(me + k, 4)}, device_id_type=MESH)

    def ret_copy(k):
        s = lax.rem(me + k, 4)
        return pltpu.make_async_remote_copy(
            src_ref=drag_s.at[pl.ds(pl.multiple_of(s * 96, 96), 96)],
            dst_ref=ret.at[pl.ds(pl.multiple_of(me * 96, 96), 96)],
            send_sem=ret_ss.at[k], recv_sem=ret_rs.at[lax.rem(4 - k, 4)],
            device_id={"gy": s}, device_id_type=MESH)

    slot_lane = lax.broadcasted_iota(I32, (1, 128), 1)

    def pack_pos(dst, at, d):
        def step(g, _):
            for u in range(8):
                m = g * 8 + u
                b = perm_s[0, d * 32 + m]
                for c in range(3):
                    dst[at, pl.ds(c * 32 + m, 1), :] = pos[c, pl.ds(b, 1), :]
            return 0

        lax.fori_loop(0, 4, step, 0)

    def pack_rest(dst, at, d):
        def step(g, _):
            for u in range(8):
                m = g * 8 + u
                b = perm_s[0, d * 32 + m]
                live = slot_lane < counts[b]
                c2 = coef[b]
                for c in range(3):
                    dst[at, pl.ds(96 + c * 32 + m, 1), :] = vel[c, pl.ds(b, 1), :]
                dst[at, pl.ds(192 + m, 1), :] = jnp.where(live, c2[0:1], 0.0)
                dst[at, pl.ds(224 + m, 1), :] = c2[1:2]
            return 0

        lax.fori_loop(0, 4, step, 0)

    def third(q):
        return 2 - q + 3 * (q // 2)

    to_smem.wait()
    ins[3].wait()

    def pack_pos_to(q, _):
        k = third(q)
        pack_pos(send, k, lax.rem(me + k, 4))
        return 0

    lax.fori_loop(0, 3, pack_pos_to, 0)
    pl.semaphore_wait(bar, 3 + (gx + n_gx - 1) // n_gx + (2 * n_gx - 2 - gx) // n_gx)

    for k in (2, 1, 3):
        lab_copy(k).start()
    for k in (1, 3, 2):
        pos_copy(k).start()
    for n in (2, 4, 5):
        ins[n].wait()

    def pack_and_send(q, _):
        k = third(q)
        pack_rest(send, k, lax.rem(me + k, 4))
        dat_copy(k).start()
        return 0

    lax.fori_loop(0, 3, pack_and_send, 0)
    pack_pos(recv, me, me)
    pack_rest(recv, me, me)

    half = lax.broadcasted_iota(I32, (16, 128), 1) < 64

    ins[6].wait()

    def spread_field(n, _):
        c = n // 8
        ex = lax.rem(n // 4, 2)
        ey = lax.rem(n, 4)
        base = (ex * 4 + ey) * 16 * 24 + c * 8
        for t in range(4):
            x = field[c, ex, ey, :, t * 128:(t + 1) * 128].astype(F32)
            y = pltpu.roll(x, 64, 1)
            fbuf[pl.ds(base + t, 16, stride=24), :] = jnp.where(half, x, y)
            fbuf[pl.ds(base + 4 + t, 16, stride=24), :] = jnp.where(half, y, x)
        return 0

    lax.fori_loop(0, 24, spread_field, 0)

    for k in (1, 3, 2):
        lab_copy(k).wait()
    labels = lab_recv[0] + lab_recv[1] + lab_recv[2] + lab_recv[3]
    g_t = jnp.broadcast_to(labels, (128, 128)).T
    gt_v[...] = g_t
    inv = jnp.max(jnp.where(g_t == lane, sub, 0), axis=0, keepdims=True)
    perm_v[2:3, :] = labels
    perm_v[3:4, :] = inv
    perm_v[4:5, :] = (inv // 32) * 96 + lax.rem(inv, 32)
    to_smem = pltpu.make_async_copy(perm_v, perm_s, sm_sem.at[0])
    to_smem.start()
    to_smem.wait()

    hp = jnp.where(has_prev, 1.0, 0.0).astype(F32)
    hn = jnp.where(has_next, 1.0, 0.0).astype(F32)

    def chunk(q, _):
        k = lax.rem((q * q + q) // 2, 4)
        s = lax.rem(me + k, 4)

        @pl.when(q > 0)
        def _():
            pos_copy(lax.rem(4 - k, 4)).wait_recv()

        def bulk(g, _):
            first = s * 32 + g * 8

            def rows_of(r):
                return recv[s, pl.ds(pl.multiple_of(r * 32 + g * 8, 8), 8), :]

            def put(ref, kind, row, v):
                ref[kind, pl.ds(first * 8 + row, 8, stride=8), :] = v

            r, sc, tc = rows_of(0), rows_of(1), rows_of(2)
            lr, ls, lt = lagrange_all(r), lagrange_all(sc), lagrange_all(tc)
            for i in range(8):
                put(lag, 0, ROW[i], lr[i])
                put(lag, 1, i, ls[i])
                put(lag, 2, i, lt[i])
            ex0 = gt_v[pl.ds(pl.multiple_of(first, 8), 8), :] < 64
            own, minus, plus = gauss_all(r), gauss_all(r + 2.0), gauss_all(r - 2.0)
            zero = jnp.zeros_like(r)
            for i in range(8):
                o, p, m, x = own[i], plus[i], minus[i], zero
                if i == 0:
                    o = o + jnp.where(ex0, hp * minus[7], minus[7])
                    p = p + own[7]
                    x = jnp.where(ex0, plus[7], 0.0)
                if i == 7:
                    o = o + jnp.where(ex0, plus[0], hn * plus[0])
                    m = m + own[0]
                    x = jnp.where(ex0, 0.0, minus[0])
                put(gau, 0, ROW[i], o)
                put(gau, 1, ROW[i], p)
                put(gau, 2, ROW[i], m)
                put(gau, 3, ROW[i], x)
            gs, gt = gauss_all(sc), gauss_all(tc)
            for i in range(8):
                put(gau, 4, i, gs[i])
                put(gau, 5, i, gt[i])
            return 0

        lax.fori_loop(0, 4, bulk, 0)

        def interp(g, _):
            for u in range(32):
                slot = s * 32 + g * 32 + u
                e = perm_s[2, slot]
                f = fbuf[pl.ds(e * 24, 24), :].astype(BF16)
                at = pl.multiple_of(slot * 8, 8)
                lt = lag[2, pl.ds(at, 8), :]
                ls = lag[1, pl.ds(at, 8), :]
                plane = jnp.concatenate([ls[j:j + 1] * lt for j in range(8)], axis=0)
                hi, lo = split_bf16(plane)
                out = jnp.dot(f, jnp.concatenate([hi, lo], axis=0), preferred_element_type=F32)
                lr = lag[0, pl.ds(at, 8), :]
                for c in range(3):
                    fluid[c, pl.ds(slot, 1), :] = jnp.sum(out[8 * c:8 * c + 8] * lr, axis=0, keepdims=True)
            return 0

        interp(0, 0)
        return 0

    lax.fori_loop(0, 4, chunk, 0)

    def drags(q, _):
        k = lax.rem((q * q + q) // 2, 4)
        s = lax.rem(me + k, 4)

        @pl.when(q > 0)
        def _():
            dat_copy(lax.rem(4 - k, 4)).wait_recv()

        rel = []
        for c in range(3):
            rel.append(fluid[c, pl.ds(pl.multiple_of(s * 32, 32), 32), :]
                       - recv[s, 96 + c * 32:128 + c * 32, :])
        speed = jnp.sqrt(rel[0] * rel[0] + rel[1] * rel[1] + rel[2] * rel[2])
        reynolds = jnp.maximum(recv[s, 224:256, :] * speed, 1e-30)
        factor = recv[s, 192:224, :] * (1.0 + 0.15 * jnp.exp(0.687 * jnp.log(reynolds)))
        for c in range(3):
            drag_s[pl.ds(pl.multiple_of(s * 96 + c * 32, 32), 32), :] = factor * rel[c]

        @pl.when(q > 0)
        def _():
            ret_copy(k).start()
        return 0

    lax.fori_loop(0, 4, drags, 0)
    own_rows = pl.ds(pl.multiple_of(me * 96, 96), 96)
    ret[own_rows, :] = drag_s[own_rows, :]

    half8 = lax.broadcasted_iota(I32, (8, 128), 1) < 64

    def gm_copy(ey):
        return pltpu.make_async_remote_copy(
            src_ref=gsend.at[0, ey], dst_ref=grecv.at[0, ey], send_sem=gm_ss.at[ey], recv_sem=gm_rs.at[ey],
            device_id={"gx": gx - 1}, device_id_type=MESH)

    def gp_copy(ey):
        return pltpu.make_async_remote_copy(
            src_ref=gsend.at[1, ey], dst_ref=grecv.at[1, ey], send_sem=gp_ss.at[ey], recv_sem=gp_rs.at[ey],
            device_id={"gx": gx + 1}, device_id_type=MESH)

    def weights(slot, drow, order):
        at = slot * 8
        gs = gau[4, pl.ds(at, 8), :]
        gt = gau[5, pl.ds(at, 8), :]
        plane = jnp.concatenate([gs[j:j + 1] * gt for j in range(8)], axis=0)
        hi, lo = split_bf16(plane)
        rhs = jnp.concatenate([hi, lo], axis=0)
        d = [jnp.broadcast_to(-drag_s[pl.ds(drow + c * 32, 1), :], (8, 128)) for c in range(3)]
        w = [gau[n, pl.ds(at, 8), :] for n in order]
        lhs = jnp.concatenate([a * d[c] for a in w for c in range(3)], axis=0)
        lhi, llo = split_bf16(lhs)
        return rhs, lhi, llo

    def deposit_row(q, _):
        ey = lax.rem(3 * q, 4)

        def pair_group(g, _):
            for u in range(16):
                ez = g * 16 + u
                e0 = ey * 16 + ez
                e1 = 64 + e0
                r0, h0, l0 = weights(perm_s[3, e0], perm_s[4, e0], (0, 1, 2, 3))
                r1, h1, l1 = weights(perm_s[3, e1], perm_s[4, e1], (2, 0, 3, 1))
                lhs = jnp.concatenate(
                    [jnp.concatenate([h0, h1], axis=1), jnp.concatenate([l0, l1], axis=1)], axis=0)
                rhs = jnp.concatenate([r0, r1], axis=1)
                out = lax.dot_general(lhs, rhs, (((1,), (1,)), ((), ())), preferred_element_type=F32)
                z = out[0:96] + out[96:192]
                z = z + pltpu.roll(z, 64, 1)
                ezh, ezl = ez // 8, ez % 8
                for o in range(4):
                    for c in range(3):
                        v = z[(o * 3 + c) * 8:(o * 3 + c) * 8 + 8]
                        v = jnp.where(half8, v, pltpu.roll(v, 4, 0))[0:4]
                        if o < 2:
                            tot[c, o, ey, pl.ds(ezh * 32 + ezl, 4, stride=8), :] = v
                        else:
                            gsend[o - 2, ey, c, pl.ds(ezh * 32 + ezl, 4, stride=8), :] = v
            return 0

        pair_group(0, 0)

        @pl.when(has_prev)
        def _():
            gm_copy(ey).start()

        @pl.when(has_next)
        def _():
            gp_copy(ey).start()
        return 0

    lax.fori_loop(0, 4, deposit_row, 0)

    for k in (1, 3, 2):
        ret_copy(k).wait()

    def unpack(g, _):
        for u in range(8):
            b = g * 8 + u
            row = perm_s[1, b]
            for c in range(3):
                drag_out[c, pl.ds(b, 1), :] = ret[pl.ds(row + c * 32, 1), :]
        return 0

    lax.fori_loop(0, 16, unpack, 0)

    drag_done = pltpu.make_async_copy(drag_out, drag_h, out_sem.at[6])
    drag_done.start()

    def z_copy(ey):
        return pltpu.make_async_copy(ztot.at[:, :, ey], ztot_h.at[:, :, ey], out_sem.at[ey])

    lane16 = lax.broadcasted_iota(I32, (16, 128), 1)
    row16 = lax.broadcasted_iota(I32, (16, 128), 0)
    j16 = lax.rem(lane16 // 8, 8)
    half16 = lane16 < 64
    k16 = lax.rem(lane16, 8)
    z_up = (k16 == 7) & (row16 < 15)
    z_down = (k16 == 0) & (row16 > 0)

    def add_ghost(q, _):
        ey = lax.rem(3 * q, 4)

        @pl.when(has_next)
        def _():
            gm_copy(ey).wait_recv()

        @pl.when(jnp.logical_not(has_next))
        def _():
            grecv[0, ey] = jnp.zeros((3, 64, 128), F32)

        @pl.when(has_prev)
        def _():
            gp_copy(ey).wait_recv()

        @pl.when(jnp.logical_not(has_prev))
        def _():
            grecv[1, ey] = jnp.zeros((3, 64, 128), F32)

        def tile(ref, t):
            return jnp.concatenate([ref[t * 8:t * 8 + 8, :], ref[32 + t * 8:40 + t * 8, :]], axis=0)

        for c in range(3):
            for t in range(4):
                up = tile(grecv.at[0, ey, c], t)
                down = tile(grecv.at[1, ey, c], t)
                if t == 0:
                    up = up + jnp.where(half16, pltpu.roll(tile(grecv.at[1, ey, c], 3), 64, 1), 0.0)
                if t == 3:
                    down = down + jnp.where(half16, 0.0, pltpu.roll(tile(grecv.at[0, ey, c], 0), 64, 1))
                for ex, ghost in ((0, down), (1, up)):
                    y = tile(tot.at[c, ex, ey], t) + ghost
                    above = pltpu.roll(pltpu.roll(y, 7, 1), 15, 0)
                    below = pltpu.roll(pltpu.roll(y, 121, 1), 1, 0)
                    y = y + jnp.where(z_up, above, jnp.where(z_down, below, 0.0))
                    ztot[c, ex, ey, t * 8:t * 8 + 8, :] = y[:8]
                    ztot[c, ex, ey, 32 + t * 8:40 + t * 8, :] = y[8:]
        z_copy(ey).start()
        return 0

    lax.fori_loop(0, 2, add_ghost, 0)

    lane8 = lax.broadcasted_iota(I32, (8, 128), 1)
    j8 = lax.rem(lane8 // 8, 8)
    for c in range(3):
        for h in range(2):
            lo_face = jnp.zeros((8, 128), F32)
            hi_face = jnp.zeros((8, 128), F32)
            for ex in range(2):
                for t in range(4):
                    n = ex * 4 + t
                    rows = slice(h * 32 + t * 8, h * 32 + t * 8 + 8)
                    lo_face = jnp.where(j8 == n, rolled(ztot[c, ex, 0, rows, :], 8 * n, 1), lo_face)
                    hi_face = jnp.where(j8 == n, rolled(ztot[c, ex, 3, rows, :], 8 * n - 56, 1), hi_face)
            ysend[0, (c * 2 + h) * 8:(c * 2 + h) * 8 + 8, :] = lo_face
            ysend[1, (c * 2 + h) * 8:(c * 2 + h) * 8 + 8, :] = hi_face

    def y_copy(way):
        return pltpu.make_async_remote_copy(
            src_ref=ysend.at[way], dst_ref=yrecv.at[way], send_sem=y_ss.at[way], recv_sem=y_rs.at[way],
            device_id={"gy": me - 1 if way == 0 else me + 1}, device_id_type=MESH)

    @pl.when(has_lo)
    def _():
        y_copy(0).start()

    @pl.when(has_hi)
    def _():
        y_copy(1).start()

    lax.fori_loop(2, 4, add_ghost, 0)

    @pl.when(has_hi)
    def _():
        y_copy(0).wait_recv()

    @pl.when(jnp.logical_not(has_hi))
    def _():
        yrecv[0] = jnp.zeros((48, 128), F32)

    @pl.when(has_lo)
    def _():
        y_copy(1).wait_recv()

    @pl.when(jnp.logical_not(has_lo))
    def _():
        yrecv[1] = jnp.zeros((48, 128), F32)

    faces = [pltpu.make_async_copy(yrecv.at[way], face_h.at[way], out_sem.at[4 + way]) for way in range(2)]
    for copy in faces:
        copy.start()

    for k in (1, 2, 3):
        pos_copy(k).wait_send()
        dat_copy(k).wait_send()

    for ey in range(4):
        @pl.when(has_prev)
        def _():
            gm_copy(ey).wait_send()

        @pl.when(has_next)
        def _():
            gp_copy(ey).wait_send()

    @pl.when(has_lo)
    def _():
        y_copy(0).wait_send()

    @pl.when(has_hi)
    def _():
        y_copy(1).wait_send()
    drag_done.wait()
    for ey in range(4):
        z_copy(ey).wait()
    for copy in faces:
        copy.wait()


def finish(drag_h, ztot_h, face_h, drag_o, src_o, drag, ztot, yrecv, src, in_sem, out_sem):
    faces_in = pltpu.make_async_copy(face_h, yrecv, in_sem.at[6])
    drag_in = pltpu.make_async_copy(drag_h, drag, in_sem.at[7])
    drag_done = pltpu.make_async_copy(drag, drag_o, out_sem.at[6])

    def z_in(n):
        return pltpu.make_async_copy(ztot_h.at[n], ztot.at[n], in_sem.at[n])

    def z_out(n):
        return pltpu.make_async_copy(src.at[n], src_o.at[n], out_sem.at[n])

    faces_in.start()
    for n in range(3):
        z_in(n).start()
    drag_in.start()
    lane16 = lax.broadcasted_iota(I32, (16, 128), 1)
    j16 = lax.rem(lane16 // 8, 8)
    faces_in.wait()
    for part in range(6):
        c, ex = part // 2, part % 2
        if ex == 0:
            z_in(c).wait()
        for t in range(4):
            n = ex * 4 + t
            lo_rows = slice(t * 8, t * 8 + 8)
            hi_rows = slice(32 + t * 8, 32 + t * 8 + 8)
            x = [jnp.concatenate([ztot[c, ex, ey, lo_rows, :], ztot[c, ex, ey, hi_rows, :]], axis=0)
                 for ey in range(4)]
            from_hi = rolled(yrecv[0, c * 16:c * 16 + 16, :], 56 - 8 * n, 1)
            from_lo = rolled(yrecv[1, c * 16:c * 16 + 16, :], -8 * n, 1)
            for ey in range(4):
                nxt = from_hi if ey == 3 else pltpu.roll(x[ey + 1], 56, 1)
                prv = from_lo if ey == 0 else pltpu.roll(x[ey - 1], 72, 1)
                src[c, ex, ey, :, t * 128:(t + 1) * 128] = x[ey] + jnp.where(
                    j16 == 7, nxt, jnp.where(j16 == 0, prv, 0.0))
        if ex == 1:
            z_out(c).start()
        if part == 1:
            drag_in.wait()
            drag_done.start()
    for n in range(3):
        z_out(n).wait()
    drag_done.wait()


def body(velocity, part_pos, part_vel, part_coef, counts, dest, elem):
    hbm = pl.BlockSpec(memory_space=pltpu.HBM)
    dma = pltpu.SemaphoreType.DMA
    drag, ztot, face = pl.pallas_call(
        kernel,
        out_shape=(
            jax.ShapeDtypeStruct((3, 128, 128), F32),
            jax.ShapeDtypeStruct((3, 2, 4, 64, 128), F32),
            jax.ShapeDtypeStruct((2, 48, 128), F32),
        ),
        in_specs=[hbm] * 7,
        out_specs=(hbm, hbm, hbm),
        scratch_shapes=[
            pltpu.VMEM((3, 2, 4, 16, 512), BF16),
            pltpu.VMEM((3, 128, 128), F32),
            pltpu.VMEM((3, 128, 128), F32),
            pltpu.VMEM((128, 2, 128), F32),
            pltpu.SMEM((128,), I32),
            pltpu.VMEM((1, 128), I32),
            pltpu.VMEM((1, 128), I32),
            dma((7,)),
            pltpu.VMEM((3, 128, 128), F32),
            dma((7,)),
            pltpu.VMEM((4, 256, 128), F32),
            pltpu.VMEM((4, 256, 128), F32),
            pltpu.VMEM((4, 1, 128), I32),
            pltpu.VMEM((4, 1, 128), I32),
            pltpu.VMEM((8, 128), I32),
            pltpu.SMEM((8, 128), I32),
            pltpu.VMEM((128, 128), I32),
            pltpu.VMEM((3072, 128), F32),
            pltpu.VMEM((3, 1024, 128), F32),
            pltpu.VMEM((6, 1024, 128), F32),
            pltpu.VMEM((3, 128, 128), F32),
            pltpu.VMEM((384, 128), F32),
            pltpu.VMEM((384, 128), F32),
            pltpu.VMEM((3, 2, 4, 64, 128), F32),
            pltpu.VMEM((3, 2, 4, 64, 128), F32),
            pltpu.VMEM((2, 4, 3, 64, 128), F32),
            pltpu.VMEM((2, 4, 3, 64, 128), F32),
            pltpu.VMEM((2, 48, 128), F32),
            pltpu.VMEM((2, 48, 128), F32),
            dma((1,)), dma((4,)), dma((4,)), dma((4,)), dma((4,)), dma((4,)), dma((4,)), dma((4,)), dma((4,)),
            dma((4,)), dma((4,)), dma((4,)), dma((4,)), dma((2,)), dma((2,)),
        ],
        compiler_params=pltpu.CompilerParams(
            collective_id=0, has_side_effects=True, vmem_limit_bytes=67043328),
    )(velocity, part_pos.transpose(1, 0, 2), part_vel.transpose(1, 0, 2), part_coef, counts,
      dest.reshape(1, 128), elem.reshape(1, 128))
    drag, source = pl.pallas_call(
        finish,
        in_specs=[hbm] * 3,
        out_specs=(hbm, hbm),
        out_shape=(
            jax.ShapeDtypeStruct((3, 128, 128), F32),
            jax.ShapeDtypeStruct(velocity.shape, F32),
        ),
        scratch_shapes=[
            pltpu.VMEM((3, 128, 128), F32),
            pltpu.VMEM((3, 2, 4, 64, 128), F32),
            pltpu.VMEM((2, 48, 128), F32),
            pltpu.VMEM(velocity.shape, F32),
            dma((8,)), dma((7,)),
        ],
        compiler_params=pltpu.CompilerParams(vmem_limit_bytes=67043328),
    )(drag, ztot, face)
    return drag.transpose(1, 0, 2), source


def solution(mesh):
    in_specs = (
        P(None, "gx", "gy", None, None),
        P(("gx", "gy"), None, None),
        P(("gx", "gy"), None, None),
        P(("gx", "gy"), None, None),
        P(("gx", "gy")),
        P(("gx", "gy")),
        P(("gx", "gy")),
    )
    out_specs = (P(("gx", "gy"), None, None), P(None, "gx", "gy", None, None))
    return jax.shard_map(body, mesh=mesh, in_specs=in_specs, out_specs=out_specs, check_vma=False)
```
